128 devices in a mesh: rep: 2 (over core), dp: 64 (over x, y, z).
Axes of the slice: x: 4, y: 4, z: 4, core: 2. Of those that a mesh axis runs over, the one named last changes fastest.
Arguments:
- x: bfloat16 [128, 1024, 640], P(('rep', 'dp')), parts along dimension 0
- dy: bfloat16 [128, 1024, 640], P(('rep', 'dp')), parts along dimension 0
- wq: bfloat16 [1, 640, 1024], replicated
- wk: bfloat16 [1, 640, 128], replicated
- wv: bfloat16 [1, 640, 128], replicated
- wo: bfloat16 [1, 1024, 640], replicated
- w_gate: bfloat16 [1, 640, 3200], replicated
- w_up: bfloat16 [1, 640, 3200], replicated
- w_down: bfloat16 [1, 3200, 640], replicated
- m_wq: float32 [1, 640, 1024], P(None, 'dp')
- m_wk: float32 [1, 640, 128], P(None, 'dp')
- m_wv: float32 [1, 640, 128], P(None, 'dp')
- m_wo: float32 [1, 1024, 640], P(None, 'dp')
- m_w_gate: float32 [1, 640, 3200], P(None, 'dp')
- m_w_up: float32 [1, 640, 3200], P(None, 'dp')
- m_w_down: float32 [1, 3200, 640], P(None, 'dp')
- v_wq: float32 [1, 640, 1024], P(None, 'dp')
- v_wk: float32 [1, 640, 128], P(None, 'dp')
- v_wv: float32 [1, 640, 128], P(None, 'dp')
- v_wo: float32 [1, 1024, 640], P(None, 'dp')
- v_w_gate: float32 [1, 640, 3200], P(None, 'dp')
- v_w_up: float32 [1, 640, 3200], P(None, 'dp')
- v_w_down: float32 [1, 3200, 640], P(None, 'dp')
Outputs:
- output 1: bfloat16 [2, 640, 1024], P('rep'), parts along dimension 0
- output 2: bfloat16 [2, 640, 128], P('rep'), parts along dimension 0
- output 3: bfloat16 [2, 640, 128], P('rep'), parts along dimension 0
- output 4: bfloat16 [2, 1024, 640], P('rep'), parts along dimension 0
- output 5: bfloat16 [2, 640, 3200], P('rep'), parts along dimension 0
- output 6: bfloat16 [2, 640, 3200], P('rep'), parts along dimension 0
- output 7: bfloat16 [2, 3200, 640], P('rep'), parts along dimension 0
- output 8: float32 [2, 640, 1024], P('rep', 'dp'), parts along dimension 0
- output 9: float32 [2, 640, 128], P('rep', 'dp'), parts along dimension 0
- output 10: float32 [2, 640, 128], P('rep', 'dp'), parts along dimension 0
- output 11: float32 [2, 1024, 640], P('rep', 'dp'), parts along dimension 0
- output 12: float32 [2, 640, 3200], P('rep', 'dp'), parts along dimension 0
- output 13: float32 [2, 640, 3200], P('rep', 'dp'), parts along dimension 0
- output 14: float32 [2, 3200, 640], P('rep', 'dp'), parts along dimension 0
- output 15: float32 [2, 640, 1024], P('rep', 'dp'), parts along dimension 0
- output 16: float32 [2, 640, 128], P('rep', 'dp'), parts along dimension 0
- output 17: float32 [2, 640, 128], P('rep', 'dp'), parts along dimension 0
- output 18: float32 [2, 1024, 640], P('rep', 'dp'), parts along dimension 0
- output 19: float32 [2, 640, 3200], P('rep', 'dp'), parts along dimension 0
- output 20: float32 [2, 640, 3200], P('rep', 'dp'), parts along dimension 0
- output 21: float32 [2, 3200, 640], P('rep', 'dp'), parts along dimension 0
There are 2 independent parts. The reference program is written for one: setup_inputs(seed, part) draws one part's arguments, and reference() takes and returns one part's arrays. A program takes and returns all parts, laid end to end along the dimension named above; an argument that names none is the same for every part.
All inputs are finite; a program needn't handle non-finite values.
Results may differ from the reference program's by a relative error of at most 0.024.
Values are sent between devices in bfloat16 or wider.
A program may use at most 1.5 GiB of HBM per device.

```python
import jax
import jax.numpy as jnp
from jax import lax

SEQUENCES = 64
TOKENS = 1024
D = 640
HEADS = 8
KV_HEADS = 1
HEAD = 128
FF = 3200
LAYERS = 1
THETA = 10000
NAMES = ("wq", "wk", "wv", "wo", "w_gate", "w_up", "w_down")
SHAPES = {
    "wq": (LAYERS, D, HEADS * HEAD),
    "wk": (LAYERS, D, KV_HEADS * HEAD),
    "wv": (LAYERS, D, KV_HEADS * HEAD),
    "wo": (LAYERS, HEADS * HEAD, D),
    "w_gate": (LAYERS, D, FF),
    "w_up": (LAYERS, D, FF),
    "w_down": (LAYERS, FF, D),
}


def bump(key, n, height):
    away = (jnp.arange(n, dtype=jnp.int32) - jax.random.randint(key, (), 0, n, jnp.int32)) % n
    return jnp.where(away < n // 8, height, 1.0)


def together(key, own, strength):
    shared = jax.random.normal(key, own.shape[1:], jnp.float32)
    return (own + strength * shared) * lax.rsqrt(1 + strength * strength)


def setup_inputs(seed: int = 0, part: int = 0) -> dict:
    kx, kdy, ka, kb, kz, kf, kh, kl, *keys = jax.random.split(jax.random.key(seed), 8 + 3 * len(NAMES))
    kx, kdy, ka, kb = (jax.random.fold_in(k, part) for k in (kx, kdy, ka, kb))
    kw, km, kv = (keys[i::3] for i in range(3))
    shape = (SEQUENCES, TOKENS, D)
    much_x, much_dy = jax.random.uniform(kz, (2,), jnp.float32, 0.0, 1.0)
    loud = 2.0 ** jax.random.uniform(jax.random.fold_in(kz, 1), (), jnp.float32, -1.0, 2.0)
    layers = 2.0 ** jax.random.uniform(kl, (LAYERS, 1, 1), jnp.float32, -1.0, 1.0)
    times = {"wq": 1.0, "wk": 1.0, "wv": 2.0, "wo": layers, "w_gate": 1.0, "w_up": bump(kh, FF, 4.0), "w_down": layers}
    x = together(ka, jax.random.normal(kx, shape, jnp.float32), much_x) * bump(kf, D, 4.0)
    dy = together(kb, jax.random.normal(kdy, shape, jnp.float32), much_dy)
    drawn = {"x": x.astype(jnp.bfloat16), "dy": (loud * dy * (SEQUENCES * TOKENS) ** -0.5).astype(jnp.bfloat16)}
    for key, name in zip(kw, NAMES, strict=True):
        drawn[name] = (jax.random.normal(key, SHAPES[name], jnp.float32) * SHAPES[name][1] ** -0.5 * times[name]).astype(jnp.bfloat16)
    for key, name in zip(km, NAMES, strict=True):
        drawn[f"m_{name}"] = 0.1 * jax.random.normal(key, SHAPES[name], jnp.float32)
    for key, name in zip(kv, NAMES, strict=True):
        drawn[f"v_{name}"] = jax.random.uniform(key, SHAPES[name], jnp.float32, 0.02, 0.06)
    return drawn


def matmul(a, w):
    return jnp.dot(a, w, preferred_element_type=jnp.float32).astype(jnp.bfloat16)


def normed(h):
    wide = h.astype(jnp.float32)
    scale = lax.rsqrt(jnp.mean(wide**2, -1, keepdims=True) + 1e-6)
    return (wide * scale).astype(jnp.bfloat16)


def turned(t, theta):
    half = t.shape[-1] // 2
    angle = jnp.arange(t.shape[0], dtype=jnp.float32)[:, None] * theta ** (-jnp.arange(half, dtype=jnp.float32) / half)
    cos, sin = jnp.cos(angle)[:, None], jnp.sin(angle)[:, None]
    a, b = t[..., :half].astype(jnp.float32), t[..., half:].astype(jnp.float32)
    return jnp.concatenate([a * cos - b * sin, b * cos + a * sin], -1).astype(jnp.bfloat16)


def seen_by(q, k, v):
    tokens, kv = q.shape[0], k.shape[1]
    q = q.reshape(tokens, kv, -1, q.shape[-1])
    scores = jnp.einsum("tgsd,ugd->gstu", q.astype(jnp.float32), k.astype(jnp.float32)) * q.shape[-1] ** -0.5
    place = jnp.arange(tokens)
    weights = jax.nn.softmax(jnp.where(place[:, None] >= place, scores, -jnp.inf), -1).astype(jnp.bfloat16)
    return jnp.einsum("gstu,ugd->tgsd", weights.astype(jnp.float32), v.astype(jnp.float32)).astype(jnp.bfloat16).reshape(tokens, -1)


def layer(h, w):
    a = normed(h)
    q, k = (turned(matmul(a, w[name]).reshape(h.shape[0], -1, HEAD), THETA) for name in ("wq", "wk"))
    h = h + matmul(seen_by(q, k, matmul(a, w["wv"]).reshape(h.shape[0], -1, HEAD)), w["wo"])
    b = normed(h)
    gate = jnp.dot(b, w["w_gate"], preferred_element_type=jnp.float32)
    up = jnp.dot(b, w["w_up"], preferred_element_type=jnp.float32)
    return h + matmul((jax.nn.silu(gate) * up).astype(jnp.bfloat16), w["w_down"])


def adamw(w, m, v, g):
    m = 0.9 * m + 0.1 * g
    v = 0.95 * v + 0.05 * g * g
    step = m * lax.rsqrt(v + 1e-8) + 0.1 * w
    return (w - 0.02 * step).astype(jnp.bfloat16), m, v


def clipped(gradients, sum_of_squares, count):
    factor = jnp.minimum(1.0, 0.5 * lax.rsqrt(sum_of_squares / count + 1e-30))
    return [g * factor for g in gradients]


def stack(weights, h):
    return lax.scan(lambda h, w: (layer(h, w), None), h, weights)[0]


def reference(x, dy, wq, wk, wv, wo, w_gate, w_up, w_down, m_wq, m_wk, m_wv, m_wo, m_w_gate, m_w_up, m_w_down, v_wq, v_wk, v_wv, v_wo, v_w_gate, v_w_up, v_w_down):
    weights = dict(zip(NAMES, (wq, wk, wv, wo, w_gate, w_up, w_down), strict=True))

    def take(so_far, sequence):
        h, by_y = sequence
        _, back = jax.vjp(stack, weights, h)
        by_weights, by_h = back(by_y)
        return jax.tree.map(lambda total, term: total + term.astype(jnp.float32), so_far, by_weights), by_h

    none_yet = {name: jnp.zeros(w.shape, jnp.float32) for name, w in weights.items()}
    by_weights, by_x = lax.scan(take, none_yet, (x, dy))
    gradients = [by_weights[name].astype(jnp.bfloat16).astype(jnp.float32) for name in NAMES]
    gradients = clipped(gradients, sum(jnp.sum(g * g) for g in gradients), sum(g.size for g in gradients))
    first = (m_wq, m_wk, m_wv, m_wo, m_w_gate, m_w_up, m_w_down)
    second = (v_wq, v_wk, v_wv, v_wo, v_w_gate, v_w_up, v_w_down)
    new = [adamw(weights[name].astype(jnp.float32), m, v, g) for name, m, v, g in zip(NAMES, first, second, gradients, strict=True)]
    return tuple(one[which] for which in range(3) for one in new)
```

```python
import functools

import jax
import jax.numpy as jnp
from jax import lax
from jax.experimental import pallas as pl
from jax.experimental.pallas import tpu as pltpu
from jax.sharding import PartitionSpec as P


NEG = -1e30
HIDDEN = 2 * NEG
LOG2E = 1.4426950408889634
VMEM = 56 * 2**20
STRIP = 512
ALL = ...
HEAD = LANES = 128
HEADS = 8
TILE = 640
SCALE = HEAD**-0.5
THETA = 10000
NAMES = ("wq", "wk", "wv", "wo", "w_gate", "w_up", "w_down")


NN, NT = (1, 0), (1, 1)


def _dot(a, b, ca, cb):
    return lax.dot_general(a, b, (((ca,), (cb,)), ((), ())), preferred_element_type=jnp.float32)


def _repeat(last, body, first=0):
    lax.fori_loop(first, last, lambda i, _: body(i), None)


def _lanes(n, tiles=1):
    return slice(n * LANES, (n + tiles) * LANES)


def _gap(bk, cols, bq):
    return lax.rem(lax.broadcasted_iota(jnp.int32, (bk, cols), 1), bq) - lax.broadcasted_iota(jnp.int32, (bk, cols), 0)


def _heads(ref):
    return [ref[:, _lanes(n)] for n in range(ref.shape[1] // HEAD)]


def _stacked(ref):
    return jnp.concatenate(_heads(ref), axis=0)


def _turned(t, cos, sin):
    t = t.astype(jnp.float32)
    return (t * cos + pltpu.roll(t, HEAD // 2, 1) * sin).astype(jnp.bfloat16)


def _setup(q_ref, k_ref, cos_ref, sin_ref, gap_s, q_s, k_s, bq, bk):
    iq = pl.program_id(0)

    @pl.when(iq == 0)
    def _():
        gap_s[ALL] = _gap(bk, HEADS * bq, bq)
        k_s[ALL] = _turned(k_ref[ALL], cos_ref[ALL], sin_ref[ALL])

    here = pl.ds(pl.multiple_of(iq * bq, bq), bq)
    cos, sin = cos_ref[here, :], sin_ref[here, :]
    for n, t in enumerate(_heads(q_ref)):
        q_s[n * bq : (n + 1) * bq, :] = _turned(t, cos, sin)
    return cos, sin, here


def _forward(q_ref, k_ref, v_ref, cos_ref, sin_ref, o_ref, lse_ref, top_s, mix_s, gap_s, q_s, k_s, *, bq, bk):
    cols, iq, e = HEADS * bq, pl.program_id(0), SCALE * LOG2E
    pieces = range(0, cols, STRIP)
    _setup(q_ref, k_ref, cos_ref, sin_ref, gap_s, q_s, k_s, bq, bk)
    top_s[ALL] = jnp.full(top_s.shape, NEG, jnp.float32)
    mix_s[ALL] = jnp.zeros_like(mix_s)
    ones = jnp.ones((8, bk), k_ref.dtype)

    def block(j, masked):
        here = pl.ds(j * bk, bk)
        scores = [_dot(k_s[here, :], q_s[at : at + STRIP, :], *NT) for at in pieces]
        weights, keeps = [], []
        for at, s in zip(pieces, scores):
            if masked:
                s = jnp.where(gap_s[:, at : at + STRIP] >= j * bk - iq * bq, s, HIDDEN)
            old = top_s[:, at : at + STRIP]
            top = jnp.maximum(old, s.max(axis=0, keepdims=True))
            top_s[:, at : at + STRIP] = top
            weights.append(jnp.exp2((s - top) * e).astype(v_ref.dtype))
            keeps.append(jnp.exp2((old - top) * e))
        values = jnp.concatenate([v_ref[here, :].T, ones], axis=0)
        for at, p, keep in zip(pieces, weights, keeps):
            mix_s[:, at : at + STRIP] = mix_s[:, at : at + STRIP] * keep + _dot(values, p, *NN)

    whole = iq * (bq // bk)
    _repeat(whole, lambda j: block(j, False))
    _repeat(whole + bq // bk, lambda j: block(j, True), whole)
    total = mix_s[HEAD : HEAD + 1, :]
    mix = (mix_s[:HEAD, :] * (1 / total)).T.astype(o_ref.dtype)
    lse = top_s[ALL] * SCALE + jnp.log(total)
    for n in range(HEADS):
        o_ref[:, _lanes(n)] = mix[n * bq : (n + 1) * bq]
        lse_ref[n : n + 1, :] = lse[:, n * bq : (n + 1) * bq]


def _backward(q_ref, k_ref, v_ref, cos_ref, sin_ref, do_ref, o_ref, lse_ref, by_ref, dq_s, dk_s, dv_s, gap_s, q_s, k_s, do_s, *, bq, bk):
    cols, iq, e, low = HEADS * bq, pl.program_id(0), SCALE * LOG2E, q_ref.dtype
    pieces = range(0, cols, STRIP)
    cos, sin, rows = _setup(q_ref, k_ref, cos_ref, sin_ref, gap_s, q_s, k_s, bq, bk)

    @pl.when(iq == 0)
    def _():
        dk_s[ALL] = jnp.zeros_like(dk_s)
        dv_s[ALL] = jnp.zeros_like(dv_s)

    dq_s[ALL] = jnp.zeros_like(dq_s)
    do_s[ALL] = _stacked(do_ref)
    lses = jnp.concatenate([lse_ref[n : n + 1, :] for n in range(HEADS)], axis=1) * LOG2E
    both = do_s[ALL].astype(jnp.float32) * _stacked(o_ref).astype(jnp.float32)
    deltas = both.T.sum(axis=0, keepdims=True)

    def block(j, masked):
        here = pl.ds(j * bk, bk)
        qs = [q_s[at : at + STRIP, :] for at in pieces]
        dos = [do_s[at : at + STRIP, :] for at in pieces]
        scores = [_dot(k_s[here, :], x, *NT) for x in qs]
        dps = [_dot(v_ref[here, :], x, *NT) for x in dos]
        for n, at in enumerate(pieces):
            p = jnp.exp2(scores[n] * e - lses[:, at : at + STRIP])
            if masked:
                p = jnp.where(gap_s[:, at : at + STRIP] >= j * bk - iq * bq, p, 0.0)
            ds = (p * (dps[n] - deltas[:, at : at + STRIP])).astype(low)
            dv_s[here, :] += _dot(p.astype(low), dos[n], *NN)
            dk_s[here, :] += _dot(ds, qs[n], *NN)
            dq_s[:, at : at + STRIP] += _dot(k_s[here, :].T, ds, *NN)

    whole = iq * (bq // bk)
    _repeat(whole, lambda j: block(j, False))
    _repeat(whole + bq // bk, lambda j: block(j, True), whole)
    dq, cols_q = (dq_s[ALL] * SCALE).T.astype(low), HEADS * HEAD
    for n in range(HEADS):
        by_ref[rows, _lanes(n)] = _turned(dq[n * bq : (n + 1) * bq], cos, -sin)

    @pl.when(iq == pl.num_programs(0) - 1)
    def _():
        by_ref[:, cols_q : cols_q + HEAD] = _turned((dk_s[ALL] * SCALE).astype(low), cos_ref[ALL], -sin_ref[ALL])
        by_ref[:, cols_q + HEAD :] = dv_s[ALL].astype(low)


def _attention_call(kernel, bq, bk, given, results, scratch):
    def spec(shape, cut):
        if cut is None:
            return pl.BlockSpec(shape, lambda i: (0,) * len(shape))
        return pl.BlockSpec((bq, shape[1]), lambda i: (i, 0)) if cut == 0 else pl.BlockSpec((shape[0], bq), lambda i: (0, i))

    tokens = given[0][0].shape[0]
    return pl.pallas_call(
        functools.partial(kernel, bq=bq, bk=bk),
        grid=(tokens // bq,),
        in_specs=[spec(a.shape, cut) for a, cut in given],
        out_specs=[spec(a.shape, cut) for a, cut in results],
        out_shape=[a for a, _ in results],
        scratch_shapes=scratch,
        compiler_params=pltpu.CompilerParams(dimension_semantics=("arbitrary",), vmem_limit_bytes=VMEM),
    )(*[a for a, _ in given])


def attend(q, k, v, cos, sin):
    bq, bk = 512, 256
    cols, like = HEADS * bq, jax.ShapeDtypeStruct
    f32 = jnp.float32
    return _attention_call(
        _forward, bq, bk, [(q, 0), (k, None), (v, None), (cos, None), (sin, None)],
        [(like(q.shape, q.dtype), 0), (like((HEADS, q.shape[0]), f32), 1)],
        [pltpu.VMEM((1, cols), f32), pltpu.VMEM((HEAD + 8, cols), f32), pltpu.VMEM((bk, cols), jnp.int32), pltpu.VMEM((cols, HEAD), q.dtype),
         pltpu.VMEM(k.shape, k.dtype)])


def attend_bwd(q, k, v, cos, sin, d_out, out, lse):
    bq = bk = 256
    cols, like = HEADS * bq, jax.ShapeDtypeStruct
    f32 = jnp.float32
    return _attention_call(
        _backward, bq, bk, [(q, 0), (k, None), (v, None), (cos, None), (sin, None), (d_out, 0), (out, 0), (lse, 1)],
        [(like((q.shape[0], q.shape[1] + 2 * HEAD), q.dtype), None)],
        [pltpu.VMEM((HEAD, cols), f32), pltpu.VMEM(k.shape, f32), pltpu.VMEM(k.shape, f32), pltpu.VMEM((bk, cols), jnp.int32),
         pltpu.VMEM((cols, HEAD), q.dtype), pltpu.VMEM(k.shape, k.dtype), pltpu.VMEM((cols, HEAD), q.dtype)])[0]


def _ffn(b_ref, dy_ref, wg_ref, wu_ref, wd_ref, act_ref, dg_ref, du_ref, db_ref, acc_g, acc_u):
    j, low = pl.program_id(0), act_ref.dtype

    @pl.when(j == 0)
    def _():
        acc_g[ALL] = jnp.zeros_like(acc_g)
        acc_u[ALL] = jnp.zeros_like(acc_u)

    def part(i):
        rows = pl.ds(pl.multiple_of(i * STRIP, STRIP), STRIP)
        gate, up = _dot(b_ref[rows, :], wg_ref[ALL], *NN), _dot(b_ref[rows, :], wu_ref[ALL], *NN)
        d = _dot(dy_ref[rows, :], wd_ref[ALL], *NT).astype(low).astype(jnp.float32)
        s = jax.nn.sigmoid(gate)
        silu = gate * s
        act_ref[rows, :] = (silu * up).astype(low)
        du, dg = (d * silu).astype(low), (d * up * (s * (1 + gate * (1 - s)))).astype(low)
        du_ref[rows, :], dg_ref[rows, :] = du, dg
        acc_g[rows, :] += _dot(dg, wg_ref[ALL], *NT)
        acc_u[rows, :] += _dot(du, wu_ref[ALL], *NT)

    _repeat(b_ref.shape[0] // STRIP, part)

    @pl.when(j == pl.num_programs(0) - 1)
    def _():
        db_ref[ALL] = acc_g[ALL].astype(low) + acc_u[ALL].astype(low)


def ffn(b, dy, w_gate, w_up, w_down):
    tokens, d = b.shape
    whole = pl.BlockSpec((tokens, d), lambda j: (0, 0))
    across, down, hidden = (pl.BlockSpec(s, m) for s, m in (
        ((d, TILE), lambda j: (0, j)), ((TILE, d), lambda j: (j, 0)), ((tokens, TILE), lambda j: (0, j))))
    units = jax.ShapeDtypeStruct((tokens, w_gate.shape[1]), b.dtype)
    return pl.pallas_call(
        _ffn,
        grid=(w_gate.shape[1] // TILE,),
        in_specs=[whole, whole, across, across, down],
        out_specs=[hidden, hidden, hidden, whole],
        out_shape=[units, units, units, jax.ShapeDtypeStruct(b.shape, b.dtype)],
        scratch_shapes=[pltpu.VMEM((tokens, d), jnp.float32)] * 2,
        compiler_params=pltpu.CompilerParams(dimension_semantics=("arbitrary",), vmem_limit_bytes=VMEM),
    )(b, dy, w_gate, w_up, w_down)


CUBE = (4, 4, 4)
AXES = (16, 4, 1)
ORDERS = ((0, 1, 2), (1, 2, 0), (2, 0, 1))
PHASES = COLOURS = (0, 1, 2)
SECTIONS = (0, 256, 512, 768)
FLAT = 960
BIG = ((0, 48, 32), (80, 32, 48), (160, 48, 48))
SMALL = ((0, 32, 32), (64, 32, 32), (LANES, 32, 32))
CUTS = (BIG, BIG, BIG, SMALL)
THIRD = FLAT // 3
PARTS = {"w_gate": (0, 250, 25), "w_up": (256, 250, 25), "w_down": (512, 250, 5), "wq": (768, 80, 8), "wk": (848, 10, 1), "wv": (864, 10, 1), "wo": (880, 80, 5)}
KEYS = 640 * 8
MESH = pl.DeviceIdType.MESH


def _where():
    me = lax.axis_index("dp")
    return me, (lax.div(me, AXES[0]), *_xy(lax.rem(me, 16)))


def _xy(q):
    return lax.div(q, 4), lax.rem(q, 4)


def _blocks(ref, fixed, row, n):
    index = [slice(None)] * 3
    for axis, i in fixed.items():
        index[axis] = i
    return ref.at[(*index, pl.ds(row, n))]


def _tail(count, names, *refs):
    r = dict(zip(names, refs))
    grad, flat, gs, sq = (r[n] for n in ("grad", "flat", "gs", "sq"))
    me, at = _where()

    def place(axis, by):
        return lax.rem(at[axis] + (by + 4), 4)

    def peer(axis, by):
        return {"dp": me + (place(axis, by) - at[axis]) * AXES[axis]}

    def push(src, dst, sems, index, axis, by):
        return pltpu.make_async_remote_copy(src_ref=src, dst_ref=dst, send_sem=r[sems + "_send"].at[index], recv_sem=r[sems + "_recv"].at[index],
                                            device_id=peer(axis, by), device_id_type=MESH)

    barrier = pltpu.get_barrier_semaphore()
    for axis in PHASES:
        for by in (1, 2, 3):
            pl.semaphore_signal(barrier, inc=1, device_id=peer(axis, by), device_id_type=MESH)

    moves = []

    def move(src, dst):
        moves.append(pltpu.make_async_copy(src, dst, r["own_sem"].at[len(moves)]))
        moves[-1].start()

    shift = {}
    for name, (row, rows, tiles) in PARTS.items():
        own_rows = rows // tiles
        first = lax.div(me * own_rows, 8) * 8
        shift[name] = me * own_rows - first
        near = r["near", name]
        move(r[name].at[pl.ds(pl.multiple_of(first, 8), near.shape[0])], near)
        for kind in "mv":
            given = r[kind, name]
            move(given, r["wo_" + kind]) if name == "wo" else move(given.at[:, 0], r[kind].at[pl.ds(row, rows)])

    def arrive():
        for copy in moves:
            copy.wait()
        for name, (row, rows, tiles) in PARTS.items():
            near, found = r["near", name], r["found"]
            for c in range(tiles):
                lanes = _lanes(c)
                found[pl.ds(c, near.shape[0], stride=tiles), :] = near[:, lanes].astype(jnp.float32)
                if name == "wo":
                    for kind in "mv":
                        r[kind][pl.ds(row + c, near.shape[0], stride=tiles), :] = r["wo_" + kind][:, lanes]
            r["own"][row : row + rows] = found[pl.ds(shift[name] * tiles, rows), :]

    stream, left, right = r["stream"], r["left"], r["right"]

    def load(ref, j, width, slot):
        return pltpu.make_async_copy(ref.at[:, pl.ds(j * width, width)], stream.at[slot, :, pl.ds(0, width)], r["stream_sem"].at[slot])

    def fixed(name, target):
        copy = pltpu.make_async_copy(r[name], target, r["fixed_sem"])
        copy.start()
        copy.wait()

    def job(name, number, width, keep_left, tiles):
        ref = r[name]
        load(ref, 0, width, 0).start()

        def step(j):
            slot = lax.rem(j, 2)

            @pl.when(j + 1 < number)
            def _():
                load(ref, j + 1, width, 1 - slot).start()

            load(ref, j, width, slot).wait()
            if keep_left:
                out = _dot(left[ALL], stream[slot, :, :width], *NN)
                base = j * (width // LANES)
            else:
                out = _dot(stream[slot, :, :width].T, right[ALL], *NN)
                base = j * (width * tiles)
            for c in range(out.shape[1] // LANES):
                flat[pl.ds(base + c, out.shape[0], stride=tiles), :] = out[:, _lanes(c)]

        _repeat(number, step)

    def pack(name, start=0):
        row, per, _ = PARTS[name]
        rows = -(-per // 16) * 16

        def four(q):
            base = pl.multiple_of(start + q * (4 * per), 8)
            for z in range(4):
                grad[*_xy(q), z, row : row + rows] = flat[pl.ds(base + per * z, rows), :].astype(jnp.bfloat16)

        _repeat(16, four)

    def take(name):
        fixed(name, stream.at[0])
        left[ALL] = stream[0].T

    def products(s):
        if s < 2:
            if s == 0:
                take("b")
            job(("by_gate", "by_up")[s], 5, TILE, True, 25)
            pack(("w_gate", "w_up")[s])
        elif s == 2:
            fixed("dy", right)
            job("act", 5, TILE, False, 5)
            pack("w_down")
        else:
            take("a")
            for j in range(2):
                copy = load(r["by_qkv"], j, TILE, j)
                copy.start()
                copy.wait()
                out = _dot(left[ALL], stream[j], *NN)
                for c in range(5):
                    n = 5 * j + c
                    flat[pl.ds(n, TILE, stride=8) if n < 8 else pl.ds(KEYS + (n - 8) * TILE, TILE), :] = out[:, _lanes(c)]
            pack("wq")
            pack("wk", KEYS)
            pack("wv", KEYS + TILE)
            fixed("by_h", right)
            job("att", 2, 512, False, 5)
            pack("wo")

    def sub(ref, c, k, i, row, n):
        if k == 1:
            return ref.at[i, :, pl.ds(row, n)] if ORDERS[c][1] < ORDERS[c][2] else ref.at[:, i, pl.ds(row, n)]
        return ref.at[i, pl.ds(row, n)]

    def term(s, c, k, by, row, n):
        axis = ORDERS[c][k]
        if k == 0:
            return _blocks(grad, {axis: place(axis, by)}, SECTIONS[s] + CUTS[s][c][0] + row, n)
        return sub(r["low", s, c, k - 1], c, k, place(axis, by), row, n)

    def exact(s, c, k, by, row, n):
        return term(s, c, k, by, row, n) if k == 0 else sub(r["sum", s, c, k - 1], c, k, place(ORDERS[c][k], by), row, n)

    def loop(shape, body):
        if not shape:
            body(())
        elif len(shape) < 2:
            _repeat(shape[0], lambda i: body((i,)))
        else:
            _repeat(shape[0] * shape[1], lambda i: body((lax.div(i, shape[1]), lax.rem(i, shape[1]))))

    copies = {}
    wide = lambda ref, index: ref[index].astype(jnp.float32)

    def send(s, c, k, name, i, src, to):
        copy = push(src, r[name, s, c, k], "sum", (s, c, k, i), ORDERS[c][k], to)
        copy.start()
        copies[s, c, k, name] = copy

    def begin(s, k):
        for c in COLOURS:
            _, na, nb = CUTS[s][c]
            for i, (name, by, row, n, to) in enumerate((("opp_a", 2, 0, na, 1), ("opp_b", 2, na, nb, -1), ("dir_b", 1, na, nb, 1), ("dir_a", -1, 0, na, -1))):
                send(s, c, k, name, i, term(s, c, k, by, row, n), to)

    def middle(s, k):
        for c in COLOURS:
            _, na, nb = CUTS[s][c]
            for i, (half, by, row, n) in enumerate((("a", 1, 0, na), ("b", -1, na, nb))):
                copies[s, c, k, "opp_" + half].wait_recv()
                came, mine, to = r["opp_" + half, s, c, k], exact(s, c, k, by, row, n), term(s, c, k, by, row, n)

                def add(index, came=came, mine=mine, to=to):
                    to[index] = (wide(mine, index) + wide(came, index)).astype(jnp.bfloat16)

                loop(came.shape[:-2], add)
                send(s, c, k, "acc_" + half, 4 + i, to, by)

    def finish(s, k):
        for c in COLOURS:
            first, na, nb = CUTS[s][c]
            for half, row, n in (("a", 0, na), ("b", na, nb)):
                copies[s, c, k, "dir_" + half].wait_recv()
                copies[s, c, k, "acc_" + half].wait_recv()
                near, far, mine = r["dir_" + half, s, c, k], r["acc_" + half, s, c, k], exact(s, c, k, 0, row, n)

                def add(index, near=near, far=far, mine=mine, row=row, n=n, c=c, first=first):
                    total = wide(mine, index) + (wide(near, index) + wide(far, index))
                    if k < 2:
                        r["sum", s, c, k][(*index, pl.ds(row, n))] = total
                        r["low", s, c, k][(*index, pl.ds(row, n))] = total.astype(jnp.bfloat16)
                    else:
                        gs[pl.ds(SECTIONS[s] + first + row, n)] = total.astype(jnp.bfloat16).astype(jnp.float32)

                loop(near.shape[:-2], add)

    flat[flat.shape[0] - 8 :] = jnp.zeros((8, LANES), jnp.float32)
    for s in range(len(SECTIONS)):
        products(s)
        if s == 0:
            pl.semaphore_wait(barrier, 9)
        begin(s, 0)
        if s:
            middle(s - 1, 0)
        if s > 1:
            finish(s - 2, 0)
            begin(s - 2, 1)
    arrive()
    for s, k, what in (
        (0, 1, middle), (2, 0, finish), (2, 1, begin), (0, 1, finish), (0, 2, begin), (3, 0, middle), (1, 1, middle), (0, 2, middle), (3, 0, finish), (3, 1, begin),
        (1, 1, finish), (1, 2, begin), (2, 1, middle), (0, 2, finish), (1, 2, middle), (2, 1, finish), (2, 2, begin), (3, 1, middle),
        (1, 2, finish), (2, 2, middle), (3, 1, finish), (3, 2, begin), (2, 2, finish), (3, 2, middle), (3, 2, finish)):
        what(s, k)

    part = jnp.zeros((1, LANES), jnp.float32)
    for row, rows, _ in PARTS.values():
        part += jnp.sum(gs[row : row + rows] * gs[row : row + rows], axis=0, keepdims=True)
    part = jnp.broadcast_to(part, (8, LANES))
    for copy in copies.values():
        copy.wait_send()
    sent = []
    for axis in PHASES:
        sq[axis, at[axis]] = part
        here = [push(sq.at[axis, at[axis]], sq.at[axis, at[axis]], "sq", (axis, by - 1), axis, by) for by in (1, 2, 3)]
        for copy in here:
            copy.start()
        for copy in here:
            copy.wait_recv()
        part = (sq[axis, 0] + sq[axis, 1]) + (sq[axis, 2] + sq[axis, 3])
        sent += here
    total = jnp.sum(part[0:1], axis=1, keepdims=True)
    factor = jnp.broadcast_to(jnp.minimum(1.0, 0.5 * lax.rsqrt(total / count + 1e-30)), (1, LANES))

    def rows_of(i):
        here = pl.ds(pl.multiple_of(i * 96, 32), 96)
        new, r["new_m"][here], r["new_v"][here] = adamw(r["own"][here], r["m"][here], r["v"][here], gs[here] * factor)
        grad[at[0], at[1], at[2], here] = new

    _repeat(FLAT // 96, rows_of)

    hops, outs = {}, []

    def piece(ref, c, k, by, half):
        known = {**{ORDERS[c][j]: at[ORDERS[c][j]] for j in range(k)}, ORDERS[c][k]: place(ORDERS[c][k], by)}
        return _blocks(ref, known, c * THIRD + (0 if half == "a" else THIRD // 2), THIRD // 2)

    def hop(c, k, i, by, half, to):
        hops[c, k, i] = push(piece(grad, c, k, by, half), piece(grad, c, k, by, half), "hop", (c, k, i), ORDERS[c][k], to)
        hops[c, k, i].start()

    def flush(c, by, half):
        copy = pltpu.make_async_copy(piece(grad, c, 0, by, half), piece(r["out"], c, 0, by, half), r["out_sem"].at[len(outs)])
        copy.start()
        outs.append(copy)

    def lead(c, k):
        for i, (half, to) in enumerate((("a", 1), ("b", -1), ("b", 1), ("a", -1))):
            hop(c, k, i, 0, half, to)

    for c in COLOURS:
        lead(c, 2)
    for k in reversed(PHASES):
        for c in COLOURS:
            hops[c, k, 0].wait_recv()
            hop(c, k, 4, -1, "a", 1)
            hops[c, k, 1].wait_recv()
            hop(c, k, 5, 1, "b", -1)
            if k == 0:
                for by, half in ((0, "a"), (0, "b"), (-1, "a"), (1, "b")):
                    flush(c, by, half)
        for c in COLOURS:
            for i, by, half in ((2, -1, "b"), (3, 1, "a"), (4, 2, "a"), (5, 2, "b")):
                hops[c, k, i].wait_recv()
                if k == 0:
                    flush(c, by, half)
            if k:
                lead(c, k - 1)
    for copy in outs:
        copy.wait()
    for copy in (*sent, *hops.values()):
        copy.wait_send()


def adamw(w, m, v, g):
    m = 0.9 * m + 0.1 * g
    v = 0.95 * v + 0.05 * g * g
    step = m * lax.rsqrt(v + 1e-8) + 0.1 * w
    return (w - 0.02 * step).astype(jnp.bfloat16), m, v


def tail(weights, m, v, **streams):
    low, f32, dma = jnp.bfloat16, jnp.float32, pltpu.SemaphoreType.DMA
    hbm, vmem = pl.BlockSpec(memory_space=pl.ANY), pl.BlockSpec(memory_space=pltpu.VMEM)
    count = float(64 * sum(one.size for one in m.values()))
    given = {**streams, **weights, **{(kind, name): one for kind, of in (("m", m), ("v", v)) for name, one in of.items()}}
    tokens = streams["a"].shape[0]
    scratch = {
        "grad": pltpu.VMEM((*CUBE, FLAT, LANES), low), "flat": pltpu.VMEM((64 * 250 + 8, LANES), f32), "gs": pltpu.VMEM((FLAT, LANES), f32),
        "sq": pltpu.VMEM((3, 4, 8, LANES), f32),
        "stream": pltpu.VMEM((2, tokens, TILE), low), "left": pltpu.VMEM((TILE, tokens), low), "right": pltpu.VMEM((tokens, TILE), low),
        "found": pltpu.VMEM((400, LANES), f32), "wo_m": pltpu.VMEM(m["wo"].shape, f32), "wo_v": pltpu.VMEM(m["wo"].shape, f32),
        "own_sem": dma((21,)), "stream_sem": dma((2,)), "fixed_sem": dma, "sum_send": dma((4, 3, 3, 6)), "sum_recv": dma((4, 3, 3, 6)),
        "hop_send": dma((3, 3, 6)), "hop_recv": dma((3, 3, 6)), "sq_send": dma((3, 3)), "sq_recv": dma((3, 3)), "out_sem": dma((24,)),
    }
    for name in ("own", "m", "v"):
        scratch[name] = pltpu.VMEM((FLAT, LANES), f32)
    for name, w in weights.items():
        scratch["near", name] = pltpu.VMEM((56 if name == "w_down" else 16, w.shape[1]), low)
    for s in range(len(SECTIONS)):
        for c in COLOURS:
            _, na, nb = CUTS[s][c]
            for k in PHASES:
                lead = CUBE[k + 1 :]
                for name in ("opp", "dir", "acc"):
                    scratch[name + "_a", s, c, k] = pltpu.VMEM((*lead, na, LANES), low)
                    scratch[name + "_b", s, c, k] = pltpu.VMEM((*lead, nb, LANES), low)
                if k < 2:
                    scratch["sum", s, c, k] = pltpu.VMEM((*lead, na + nb, LANES), f32)
                    scratch["low", s, c, k] = pltpu.VMEM((*lead, na + nb, LANES), low)
    moment = jax.ShapeDtypeStruct((FLAT, LANES), f32)
    return pl.pallas_call(
        functools.partial(_tail, count, [*given, "out", "new_m", "new_v", *scratch]),
        in_specs=[hbm] * len(given),
        out_specs=[hbm, vmem, vmem],
        out_shape=[jax.ShapeDtypeStruct((*CUBE, FLAT, LANES), low), moment, moment],
        scratch_shapes=list(scratch.values()),
        compiler_params=pltpu.CompilerParams(collective_id=0, has_side_effects=True, vmem_limit_bytes=67_000_000),
    )(*given.values())


def _spread(flat_in, m_in, v_in, *refs):
    outs, (came, flat, wide, high, qkv, moment, in_sem, out_sem, moment_sem) = refs[:21], refs[21:]

    def fetch(i, row, rows):
        rows = -(-rows // 16) * 16
        return pltpu.make_async_copy(flat_in.at[:, :, :, pl.ds(row, rows)], came.at[i % 2, :, :, :, pl.ds(0, rows)], in_sem.at[i % 2])

    parts = list(PARTS.items())
    copies = []

    def give(src, dst, sem):
        copies.append(pltpu.make_async_copy(src, dst, sem))
        copies[-1].start()

    fetch(0, *parts[0][1][:2]).start()
    for i, (name, (row, per, tiles)) in enumerate(parts):
        for kind, ref in enumerate((m_in, v_in)):
            out = outs[7 * (kind + 1) + i]
            if name == "wo":
                for c in range(tiles):
                    moment[kind, :, _lanes(c)] = ref[pl.ds(row + c, out.shape[0], stride=tiles), :]
                give(moment.at[kind], out, moment_sem.at[kind, i])
            else:
                give(ref.at[pl.ds(row, per)], out.at[:, 0], moment_sem.at[kind, i])
    for i, (name, (row, per, tiles)) in enumerate(parts):
        if i + 1 < len(parts):
            fetch(i + 1, *parts[i + 1][1][:2]).start()
        fetch(i, row, per).wait()

        def four(q, i=i, per=per):
            base = pl.multiple_of(q * (4 * per), 8)
            for z in range(4):
                flat[pl.ds(base + per * z, per), :] = came[i % 2, *_xy(q), z, :per].astype(jnp.float32)

        _repeat(16, four)
        rows = outs[i].shape[0]
        first = {"wk": 8, "wv": 9}.get(name, 0)
        buf = {"w_gate": wide.at[0], "w_up": wide.at[1], "w_down": high.at[0], "wo": high.at[1, :rows]}.get(name, qkv)
        step = TILE if rows % TILE == 0 else 512

        def gather(j, buf=buf, tiles=tiles, step=step, first=first):
            at = pl.multiple_of(j * step, step)
            for c in range(tiles):
                buf[pl.ds(at, step), _lanes(first + c)] = flat[pl.ds(at * tiles + c, step, stride=tiles), :].astype(jnp.bfloat16)

        _repeat(rows // step, gather)
        give(buf.at[:, _lanes(first, tiles)], outs[i], out_sem.at[i])
    for copy in copies:
        copy.wait()


def spread(flat, new_m, new_v, weights, m):
    low, f32, dma = jnp.bfloat16, jnp.float32, pltpu.SemaphoreType.DMA
    hbm, vmem = pl.BlockSpec(memory_space=pl.ANY), pl.BlockSpec(memory_space=pltpu.VMEM)
    shapes = [jax.ShapeDtypeStruct(weights[n].shape, low) for n in PARTS] + [jax.ShapeDtypeStruct(m[n].shape, f32) for n in PARTS] * 2
    d, units = weights["w_gate"].shape
    return pl.pallas_call(
        _spread,
        in_specs=[hbm, vmem, vmem],
        out_specs=[hbm] * len(shapes),
        out_shape=shapes,
        scratch_shapes=[pltpu.VMEM((2, *CUBE, 256, LANES), low), pltpu.VMEM((64 * 250, LANES), f32), pltpu.VMEM((2, d, units), low),
                        pltpu.VMEM((2, units, d), low), pltpu.VMEM((d, 2 * TILE), low), pltpu.VMEM((2, *m["wo"].shape), f32),
                        dma((2,)), dma((7,)), dma((2, 7))],
        compiler_params=pltpu.CompilerParams(vmem_limit_bytes=64_000_000),
    )(flat, new_m, new_v)


def matmul(a, w):
    return _dot(a, w, *NN).astype(jnp.bfloat16)


def normed(h):
    wide = h.astype(jnp.float32)
    scale = lax.rsqrt(jnp.mean(wide**2, -1, keepdims=True) + 1e-6)
    return (wide * scale).astype(jnp.bfloat16)


def angles(tokens):
    half = HEAD // 2
    angle = jnp.arange(tokens, dtype=jnp.float32)[:, None] * THETA ** (-jnp.arange(half, dtype=jnp.float32) / half)
    cos, sin = jnp.cos(angle), jnp.sin(angle)
    return jnp.concatenate([cos, cos], axis=1), jnp.concatenate([-sin, sin], axis=1)


def solution(mesh):
    def step(x, dy, *arrays):
        w, m, v = (dict(zip(NAMES, (one[0] for one in arrays[i : i + 7]))) for i in (0, 7, 14))
        x, dy = x[0], dy[0]
        a = normed(x)
        heads = (*(matmul(a, w[n]) for n in ("wq", "wk", "wv")), *angles(x.shape[0]))
        att, lse = attend(*heads)
        h = x + matmul(att, w["wo"])
        b, b_back = jax.vjp(normed, h)
        act, by_gate, by_up, by_b = ffn(b, dy, w["w_gate"], w["w_up"], w["w_down"])
        by_h = dy + b_back(by_b)[0]
        by_qkv = attend_bwd(*heads, _dot(by_h, w["wo"], *NT).astype(jnp.bfloat16), att, lse)

        lined = lambda of: {n: one if n == "wo" else one.reshape(-1, 1, LANES) for n, one in of.items()}
        m_lined = lined(m)
        flat = tail({n: w[n] for n in PARTS}, m_lined, lined(v), a=a, b=b, act=act, att=att, dy=dy, by_h=by_h, by_gate=by_gate, by_up=by_up, by_qkv=by_qkv)
        outs = spread(*flat, w, m_lined)
        new = [dict(zip(PARTS, outs[i : i + 7])) for i in (0, 7, 14)]
        return tuple(one[n].reshape(1, *like[n].shape) for one, like in zip(new, (w, m, m)) for n in NAMES)

    states, all_of, cut = P(("rep", "dp")), P(), P(None, "dp")
    return jax.shard_map(
        step,
        mesh=mesh,
        in_specs=(states, states) + (all_of,) * 7 + (cut,) * 14,
        out_specs=(P("rep"),) * 7 + (P("rep", "dp"),) * 14,
        check_vma=False,
    )
```

```python
import functools

import jax
import jax.numpy as jnp
import numpy as np
from jax import lax
from jax.experimental import pallas as pl
from jax.experimental.pallas import tpu as pltpu
from jax.sharding import PartitionSpec as P


NEG = -1e30
HIDDEN = 2 * NEG
LOG2E = 1.4426950408889634
VMEM = 56 * 2**20
STRIP = 512
CHUNK = 256
ALL = ...
HEAD = LANES = 128
HEADS = 8
TILE = 640
SCALE = HEAD**-0.5
THETA = 10000
NAMES = ("wq", "wk", "wv", "wo", "w_gate", "w_up", "w_down")


NN, NT = (1, 0), (1, 1)


def _dot(a, b, ca, cb):
    return lax.dot_general(a, b, (((ca,), (cb,)), ((), ())), preferred_element_type=jnp.float32)


def _repeat(last, body, first=0):
    lax.fori_loop(first, last, lambda i, _: body(i), None)


def _lanes(n, tiles=1):
    return slice(n * LANES, (n + tiles) * LANES)


def _gap(bk, cols, bq):
    return lax.rem(lax.broadcasted_iota(jnp.int32, (bk, cols), 1), bq) - lax.broadcasted_iota(jnp.int32, (bk, cols), 0)


def _heads(ref):
    return [ref[:, _lanes(n)] for n in range(ref.shape[1] // HEAD)]


def _stacked(ref):
    return jnp.concatenate(_heads(ref), axis=0)


def _turned(t, cos, sin):
    t = t.astype(jnp.float32)
    return (t * cos + pltpu.roll(t, HEAD // 2, 1) * sin).astype(jnp.bfloat16)


def _setup(k, cos_ref, sin_ref, gap_s, k_s, bq, bk):
    gap_s[ALL] = _gap(bk, HEADS * bq, bq)
    k_s[ALL] = _turned(k, cos_ref[ALL], sin_ref[ALL])


def _queries(q, cos_ref, sin_ref, q_s, bq):
    here = pl.ds(pl.multiple_of(pl.program_id(0) * bq, bq), bq)
    cos, sin = cos_ref[here, :], sin_ref[here, :]
    for n, t in enumerate(_heads(q)):
        q_s[n * bq : (n + 1) * bq, :] = _turned(t, cos, sin)
    return cos, sin, here


def _normed(h):
    wide = h.astype(jnp.float32)
    scale = lax.rsqrt(jnp.mean(wide * wide, -1, keepdims=True) + 1e-6)
    return wide, scale


def _front(x_ref, wq_ref, wk_ref, wv_ref, wo_ref, few_ref, a_ref, q_ref, k_ref, v_ref, cos_ref, sin_ref, h_ref, b_ref, o_ref, lse_ref,
           top_s, mix_s, gap_s, q_s, k_s, *, bq, bk):
    cols, iq, e, low = HEADS * bq, pl.program_id(0), SCALE * LOG2E, x_ref.dtype
    pieces = range(0, cols, STRIP)

    @pl.when(iq == 0)
    def _():
        few = few_ref.shape[1]
        for n in range(a_ref.shape[0] // few):
            cos, sin = few_ref[0, n : n + 1], few_ref[1, n : n + 1]
            cos_ref[n * few : (n + 1) * few, :] = cos * few_ref[2] - sin * few_ref[3]
            sin_ref[n * few : (n + 1) * few, :] = sin * few_ref[2] + cos * few_ref[3]
        half = lax.broadcasted_iota(jnp.int32, sin_ref.shape, 1) < HEAD // 2
        sin_ref[ALL] = jnp.where(half, -sin_ref[ALL], sin_ref[ALL])
        wide, scale = _normed(x_ref[ALL])
        a_ref[ALL] = (wide * scale).astype(low)
        k = _dot(a_ref[ALL], wk_ref[ALL], *NN).astype(low)
        k_ref[ALL] = k
        v_ref[ALL] = _dot(a_ref[ALL], wv_ref[ALL], *NN).astype(low)
        _setup(k, cos_ref, sin_ref, gap_s, k_s, bq, bk)

    rows = pl.ds(pl.multiple_of(iq * bq, bq), bq)
    q_ref[ALL] = _dot(a_ref[rows, :], wq_ref[ALL], *NN).astype(low)
    _queries(q_ref, cos_ref, sin_ref, q_s, bq)
    top_s[ALL] = jnp.full(top_s.shape, NEG, jnp.float32)
    mix_s[ALL] = jnp.zeros_like(mix_s)
    ones = jnp.ones((8, bk), k_ref.dtype)

    def block(j, masked):
        here = pl.ds(j * bk, bk)
        scores = [_dot(k_s[here, :], q_s[at : at + STRIP, :], *NT) for at in pieces]
        weights, keeps = [], []
        for at, s in zip(pieces, scores):
            if masked:
                s = jnp.where(gap_s[:, at : at + STRIP] >= j * bk - iq * bq, s, HIDDEN)
            old = top_s[:, at : at + STRIP]
            top = jnp.maximum(old, s.max(axis=0, keepdims=True))
            top_s[:, at : at + STRIP] = top
            weights.append(jnp.exp2((s - top) * e).astype(v_ref.dtype))
            keeps.append(jnp.exp2((old - top) * e))
        values = jnp.concatenate([v_ref[here, :].T, ones], axis=0)
        for at, p, keep in zip(pieces, weights, keeps):
            mix_s[:, at : at + STRIP] = mix_s[:, at : at + STRIP] * keep + _dot(values, p, *NN)

    whole = iq * (bq // bk)
    _repeat(whole, lambda j: block(j, False))
    _repeat(whole + bq // bk, lambda j: block(j, True), whole)
    total = mix_s[HEAD : HEAD + 1, :]
    mix = (mix_s[:HEAD, :] * (1 / total)).T.astype(o_ref.dtype)
    lse = top_s[ALL] * SCALE + jnp.log(total)
    for n in range(HEADS):
        o_ref[:, _lanes(n)] = mix[n * bq : (n + 1) * bq]
        lse_ref[n : n + 1, :] = lse[:, n * bq : (n + 1) * bq]
    h = x_ref[rows, :] + _dot(o_ref[ALL], wo_ref[ALL], *NN).astype(low)
    h_ref[ALL] = h
    wide, scale = _normed(h)
    b_ref[ALL] = (wide * scale).astype(low)


def _backward(q_ref, k_ref, v_ref, cos_ref, sin_ref, do_ref, o_ref, lse_ref, by_ref, dq_s, dk_s, dv_s, gap_s, q_s, k_s, do_s, *, bq, bk):
    cols, iq, e, low = HEADS * bq, pl.program_id(0), SCALE * LOG2E, q_ref.dtype
    pieces = range(0, cols, STRIP)
    cos, sin, rows = _queries(q_ref, cos_ref, sin_ref, q_s, bq)

    @pl.when(iq == 0)
    def _():
        _setup(k_ref[ALL], cos_ref, sin_ref, gap_s, k_s, bq, bk)
        dk_s[ALL] = jnp.zeros_like(dk_s)
        dv_s[ALL] = jnp.zeros_like(dv_s)

    dq_s[ALL] = jnp.zeros_like(dq_s)
    do_s[ALL] = _stacked(do_ref)
    lses = jnp.concatenate([lse_ref[n : n + 1, :] for n in range(HEADS)], axis=1) * LOG2E
    both = do_s[ALL].astype(jnp.float32) * _stacked(o_ref).astype(jnp.float32)
    deltas = both.T.sum(axis=0, keepdims=True)

    def block(j, masked):
        here = pl.ds(j * bk, bk)
        qs = [q_s[at : at + STRIP, :] for at in pieces]
        dos = [do_s[at : at + STRIP, :] for at in pieces]
        scores = [_dot(k_s[here, :], x, *NT) for x in qs]
        dps = [_dot(v_ref[here, :], x, *NT) for x in dos]
        for n, at in enumerate(pieces):
            p = jnp.exp2(scores[n] * e - lses[:, at : at + STRIP])
            if masked:
                p = jnp.where(gap_s[:, at : at + STRIP] >= j * bk - iq * bq, p, 0.0)
            ds = (p * (dps[n] - deltas[:, at : at + STRIP])).astype(low)
            dv_s[here, :] += _dot(p.astype(low), dos[n], *NN)
            dk_s[here, :] += _dot(ds, qs[n], *NN)
            dq_s[:, at : at + STRIP] += _dot(k_s[here, :].T, ds, *NN)

    whole = iq * (bq // bk)
    _repeat(whole, lambda j: block(j, False))
    _repeat(whole + bq // bk, lambda j: block(j, True), whole)
    dq, cols_q = (dq_s[ALL] * SCALE).T.astype(low), HEADS * HEAD
    for n in range(HEADS):
        by_ref[rows, _lanes(n)] = _turned(dq[n * bq : (n + 1) * bq], cos, -sin)

    @pl.when(iq == pl.num_programs(0) - 1)
    def _():
        by_ref[:, cols_q : cols_q + HEAD] = _turned((dk_s[ALL] * SCALE).astype(low), cos_ref[ALL], -sin_ref[ALL])
        by_ref[:, cols_q + HEAD :] = dv_s[ALL].astype(low)


def _attention_call(kernel, bq, bk, given, results, scratch):
    def spec(shape, cut):
        if cut is None:
            return pl.BlockSpec(shape, lambda i: (0,) * len(shape))
        return pl.BlockSpec((bq, shape[1]), lambda i: (i, 0)) if cut == 0 else pl.BlockSpec((shape[0], bq), lambda i: (0, i))

    tokens = given[0][0].shape[0]
    return pl.pallas_call(
        functools.partial(kernel, bq=bq, bk=bk),
        grid=(tokens // bq,),
        in_specs=[spec(a.shape, cut) for a, cut in given],
        out_specs=[spec(a.shape, cut) for a, cut in results],
        out_shape=[a for a, _ in results],
        scratch_shapes=scratch,
        compiler_params=pltpu.CompilerParams(dimension_semantics=("arbitrary",), vmem_limit_bytes=VMEM),
    )(*[a for a, _ in given])


def angles(tokens):
    few = int(tokens**0.5)
    turn = np.tile(THETA ** (-np.arange(HEAD // 2) / (HEAD // 2)), 2)
    far, near = (np.arange(few)[:, None] * turn * by for by in (few, 1))
    return np.stack([np.cos(far), np.sin(far), np.cos(near), np.sin(near)]).astype(np.float32)


def front(x, wq, wk, wv, wo):
    bq, bk = 512, 256
    tokens, d = x.shape
    cols, f32 = HEADS * bq, jnp.float32
    like = lambda n, t=x.dtype: jax.ShapeDtypeStruct((tokens, n), t)
    return _attention_call(
        _front, bq, bk, [(one, None) for one in (x, wq, wk, wv, wo, angles(tokens))],
        [(like(d), None), (like(wq.shape[1]), 0), (like(HEAD), None), (like(HEAD), None), (like(HEAD, f32), None), (like(HEAD, f32), None),
         (like(d), 0), (like(d), 0), (like(wo.shape[0]), 0), (jax.ShapeDtypeStruct((HEADS, tokens), f32), 1)],
        [pltpu.VMEM((1, cols), f32), pltpu.VMEM((HEAD + 8, cols), f32), pltpu.VMEM((bk, cols), jnp.int32), pltpu.VMEM((cols, HEAD), x.dtype),
         pltpu.VMEM((tokens, HEAD), x.dtype)])


def attend_bwd(q, k, v, cos, sin, d_out, out, lse):
    bq = bk = 256
    cols, like = HEADS * bq, jax.ShapeDtypeStruct
    f32 = jnp.float32
    return _attention_call(
        _backward, bq, bk, [(q, 0), (k, None), (v, None), (cos, None), (sin, None), (d_out, 0), (out, 0), (lse, 1)],
        [(like((q.shape[0], q.shape[1] + 2 * HEAD), q.dtype), None)],
        [pltpu.VMEM((HEAD, cols), f32), pltpu.VMEM(k.shape, f32), pltpu.VMEM(k.shape, f32), pltpu.VMEM((bk, cols), jnp.int32),
         pltpu.VMEM((cols, HEAD), q.dtype), pltpu.VMEM(k.shape, k.dtype), pltpu.VMEM((cols, HEAD), q.dtype)])[0]


def _ffn(b_ref, h_ref, dy_ref, wg_ref, wu_ref, wd_ref, wo_ref, act_ref, dg_ref, du_ref, dh_ref, do_ref, acc_g, acc_u):
    j, low = pl.program_id(0), act_ref.dtype

    @pl.when(j == 0)
    def _():
        acc_g[ALL] = jnp.zeros_like(acc_g)
        acc_u[ALL] = jnp.zeros_like(acc_u)

    def part(i):
        rows = pl.ds(i * CHUNK, CHUNK)
        gate, up = _dot(b_ref[rows, :], wg_ref[ALL], *NN), _dot(b_ref[rows, :], wu_ref[ALL], *NN)
        d = _dot(dy_ref[rows, :], wd_ref[ALL], *NT).astype(low).astype(jnp.float32)
        s = jax.nn.sigmoid(gate)
        silu = gate * s
        act_ref[rows, :] = (silu * up).astype(low)
        du, dg = (d * silu).astype(low), (d * up * (s * (1 + gate * (1 - s)))).astype(low)
        du_ref[rows, :], dg_ref[rows, :] = du, dg
        acc_g[rows, :] += _dot(dg, wg_ref[ALL], *NT)
        acc_u[rows, :] += _dot(du, wu_ref[ALL], *NT)

    def end(i):
        rows = pl.ds(i * CHUNK, CHUNK)
        d = (acc_g[rows, :].astype(low) + acc_u[rows, :].astype(low)).astype(jnp.float32)
        wide, scale = _normed(h_ref[rows, :])
        along = jnp.mean(d * wide, -1, keepdims=True) * (scale * scale * scale)
        dh_ref[rows, :] = dy_ref[rows, :] + (d * scale - wide * along).astype(low)
        do_ref[rows, :] = _dot(dh_ref[rows, :], wo_ref[ALL], *NT).astype(low)

    parts = b_ref.shape[0] // CHUNK
    for i in range(parts):
        part(i)

    @pl.when(j == pl.num_programs(0) - 1)
    def _():
        for i in range(parts):
            end(i)


def ffn(b, h, dy, w_gate, w_up, w_down, wo):
    tokens, d = b.shape
    whole, heads = (pl.BlockSpec((tokens, n), lambda j: (0, 0)) for n in (d, wo.shape[0]))
    across, down, hidden = (pl.BlockSpec(s, m) for s, m in (
        ((d, TILE), lambda j: (0, j)), ((TILE, d), lambda j: (j, 0)), ((tokens, TILE), lambda j: (0, j))))
    like = lambda n: jax.ShapeDtypeStruct((tokens, n), b.dtype)
    return pl.pallas_call(
        _ffn,
        grid=(w_gate.shape[1] // TILE,),
        in_specs=[whole] * 3 + [across, across, down, pl.BlockSpec(wo.shape, lambda j: (0, 0))],
        out_specs=[hidden] * 3 + [whole, heads],
        out_shape=[like(w_gate.shape[1])] * 3 + [like(d), like(wo.shape[0])],
        scratch_shapes=[pltpu.VMEM((tokens, d), jnp.float32)] * 2,
        compiler_params=pltpu.CompilerParams(dimension_semantics=("arbitrary",), vmem_limit_bytes=VMEM),
    )(b, h, dy, w_gate, w_up, w_down, wo)


CUBE = (4, 4, 4)
AXES = (16, 4, 1)
ORDERS = ((0, 1, 2), (1, 2, 0), (2, 0, 1))
PHASES = COLOURS = (0, 1, 2)
SECTIONS = (0, 256, 512, 768)
FLAT = 960
SMALL = ((0, 32, 32), (64, 32, 32), (128, 32, 32))
BIG = ((0, 48, 48), (96, 48, 32), (176, 32, 48))
CUTS = (BIG, (BIG[2], BIG[0], BIG[1]), (BIG[1], BIG[2], BIG[0]), SMALL)
THIRD = FLAT // 3
PARTS = {"w_gate": (0, 250, 25), "w_up": (256, 250, 25), "w_down": (512, 250, 5), "wq": (768, 80, 8), "wk": (848, 10, 1), "wv": (864, 10, 1), "wo": (880, 80, 5)}
KEYS = 640 * 8
MESH = pl.DeviceIdType.MESH


def _where():
    me = lax.axis_index("dp")
    return me, (lax.div(me, AXES[0]), *_xy(lax.rem(me, 16)))


def _xy(q):
    return lax.div(q, 4), lax.rem(q, 4)


def _blocks(ref, fixed, row, n):
    index = [slice(None)] * 3
    for axis, i in fixed.items():
        index[axis] = i
    return ref.at[(*index, pl.ds(row, n))]


def _tail(count, names, *refs):
    r = dict(zip(names, refs))
    grad, flat, gs, sq = (r[n] for n in ("grad", "flat", "gs", "sq"))
    me, at = _where()

    def place(axis, by):
        return lax.rem(at[axis] + (by + 4), 4)

    def peer(axis, by):
        return {"dp": me + (place(axis, by) - at[axis]) * AXES[axis]}

    def push(src, dst, sems, index, axis, by):
        return pltpu.make_async_remote_copy(src_ref=src, dst_ref=dst, send_sem=r[sems + "_send"].at[index], recv_sem=r[sems + "_recv"].at[index],
                                            device_id=peer(axis, by), device_id_type=MESH)

    barrier = pltpu.get_barrier_semaphore()
    for axis in PHASES:
        for by in (1, 2, 3):
            pl.semaphore_signal(barrier, inc=1, device_id=peer(axis, by), device_id_type=MESH)

    moves = []

    def move(src, dst):
        moves.append(pltpu.make_async_copy(src, dst, r["own_sem"].at[len(moves)]))
        moves[-1].start()

    shift = {}
    for name, (row, rows, tiles) in PARTS.items():
        own_rows = rows // tiles
        first = lax.div(me * own_rows, 8) * 8
        shift[name] = me * own_rows - first
        near = r["near", name]
        move(r[name].at[pl.ds(pl.multiple_of(first, 8), near.shape[0])], near)
        for kind in "mv":
            given = r[kind, name]
            move(given, r["wo_" + kind]) if name == "wo" else move(given.at[:, 0], r[kind].at[pl.ds(row, rows)])

    def arrive():
        for copy in moves:
            copy.wait()
        for name, (row, rows, tiles) in PARTS.items():
            near, found = r["near", name], r["found"]
            for c in range(tiles):
                lanes = _lanes(c)
                found[pl.ds(c, near.shape[0], stride=tiles), :] = near[:, lanes].astype(jnp.float32)
                if name == "wo":
                    for kind in "mv":
                        r[kind][pl.ds(row + c, near.shape[0], stride=tiles), :] = r["wo_" + kind][:, lanes]
            r["own"][row : row + rows] = found[pl.ds(shift[name] * tiles, rows), :]

    stream, left, right, spare = r["stream"], r["left"], r["right"], r["spare"]
    JOBS = (("by_gate", 5, TILE), ("by_up", 5, TILE), ("act", 5, TILE), ("by_qkv", 2, TILE), ("att", 2, 512))

    def load(i, j, slot):
        name, _, width = JOBS[i]
        return pltpu.make_async_copy(r[name].at[:, pl.ds(j * width, width)], stream.at[slot, :, pl.ds(0, width)], r["stream_sem"].at[slot])

    def fetch(name, target, sem):
        copy = pltpu.make_async_copy(r[name], target, r["fixed_sem"].at[sem])
        copy.start()
        return copy

    def each(i, use):
        number, before = JOBS[i][1], sum(n for _, n, _ in JOBS[:i])

        def step(j):
            slot = lax.rem(before + j, 2)

            @pl.when(j + 1 < number)
            def _():
                load(i, j + 1, 1 - slot).start()

            if i + 1 < len(JOBS):
                @pl.when(j + 1 == number)
                def _():
                    load(i + 1, 0, 1 - slot).start()

            load(i, j, slot).wait()
            use(j, stream[slot, :, : JOBS[i][2]])

        _repeat(number, step)

    def job(i, keep_left, tiles):
        width = JOBS[i][2]

        def use(j, tile):
            if keep_left:
                out, base = _dot(left[ALL], tile, *NN), j * (width // LANES)
            else:
                out, base = _dot(tile.T, right[ALL], *NN), j * (width * tiles)
            for c in range(out.shape[1] // LANES):
                flat[pl.ds(base + c, out.shape[0], stride=tiles), :] = out[:, _lanes(c)]

        each(i, use)

    def pack(name, start=0):
        row, per, _ = PARTS[name]
        rows = -(-per // 16) * 16

        def four(q):
            base = pl.multiple_of(start + q * (4 * per), 8)
            for z in range(4):
                grad[*_xy(q), z, row : row + rows] = flat[pl.ds(base + per * z, rows), :].astype(jnp.bfloat16)

        _repeat(16, four)

    coming = [fetch("b", spare, 0), fetch("dy", right, 1)]
    load(0, 0, 0).start()

    def products(s):
        if s < 2:
            if s == 0:
                coming[0].wait()
                left[ALL] = spare[ALL].T
                coming.append(fetch("a", spare, 0))
            job(s, True, 25)
            pack(("w_gate", "w_up")[s])
        elif s == 2:
            coming[1].wait()
            job(s, False, 5)
            coming.append(fetch("by_h", right, 1))
            pack("w_down")
        else:
            coming[2].wait()
            left[ALL] = spare[ALL].T

            def use(j, tile):
                out = _dot(left[ALL], tile, *NN)
                for c in range(3):
                    flat[pl.ds(5 * j + c, TILE, stride=8), :] = out[:, _lanes(c)]
                for c in (3, 4):
                    @pl.when(j == 0)
                    def _(c=c):
                        flat[pl.ds(c, TILE, stride=8), :] = out[:, _lanes(c)]

                    @pl.when(j > 0)
                    def _(c=c):
                        flat[pl.ds(KEYS + (c - 3) * TILE, TILE), :] = out[:, _lanes(c)]

            each(s, use)
            pack("wq")
            pack("wk", KEYS)
            pack("wv", KEYS + TILE)
            coming[3].wait()
            job(s + 1, False, 5)
            pack("wo")

    def term(s, c, k, by, row, n):
        known = {ORDERS[c][j]: at[ORDERS[c][j]] for j in range(k)}
        return _blocks(grad, {**known, ORDERS[c][k]: place(ORDERS[c][k], by)}, SECTIONS[s] + CUTS[s][c][0] + row, n)

    def exact(s, c, k, by, row, n):
        if k == 0:
            return term(s, c, k, by, row, n)
        i, here, ref = place(ORDERS[c][k], by), pl.ds(row, n), r["sum", s, c, k - 1]
        if k == 1 and ORDERS[c][1] > ORDERS[c][2]:
            return ref.at[:, i, here]
        return ref.at[i, :, here] if k == 1 else ref.at[i, here]

    def loop(ref, body):
        if len(ref.shape) > 3:
            _repeat(ref.shape[0], lambda i: body((i,)))
        else:
            body(())

    copies = {}
    wide = lambda ref, index: ref[index].astype(jnp.float32)

    def send(s, c, k, name, i, src, to):
        copy = push(src, r[name, s, c, k], "sum", (s, c, k, i), ORDERS[c][k], to)
        copy.start()
        copies[s, c, k, name] = copy

    def begin(s, k):
        for c in COLOURS:
            _, na, nb = CUTS[s][c]
            for i, (name, by, row, n, to) in enumerate((("opp_a", 2, 0, na, 1), ("opp_b", 2, na, nb, -1), ("dir_b", 1, na, nb, 1), ("dir_a", -1, 0, na, -1))):
                send(s, c, k, name, i, term(s, c, k, by, row, n), to)

    def middle(s, k):
        for c in COLOURS:
            _, na, nb = CUTS[s][c]
            for i, (half, by, row, n) in enumerate((("a", 1, 0, na), ("b", -1, na, nb))):
                copies[s, c, k, "opp_" + half].wait_recv()
                came, mine, to = r["opp_" + half, s, c, k], exact(s, c, k, by, row, n), term(s, c, k, by, row, n)

                def add(index, came=came, mine=mine, to=to):
                    to[index] = (wide(mine, index) + wide(came, index)).astype(jnp.bfloat16)

                loop(came, add)
                send(s, c, k, "acc_" + half, 4 + i, to, by)

    def finish(s, k):
        for c in COLOURS:
            first, na, nb = CUTS[s][c]
            for half, row, n in (("a", 0, na), ("b", na, nb)):
                copies[s, c, k, "dir_" + half].wait_recv()
                copies[s, c, k, "acc_" + half].wait_recv()
                near, far, mine, low = r["dir_" + half, s, c, k], r["acc_" + half, s, c, k], exact(s, c, k, 0, row, n), term(s, c, k, 0, row, n)

                def add(index, near=near, far=far, mine=mine, low=low, row=row, n=n, c=c, first=first):
                    total = wide(mine, index) + (wide(near, index) + wide(far, index))
                    if k < 2:
                        r["sum", s, c, k].at[(slice(None),) * (2 - k) + (pl.ds(row, n),)][index] = total
                        low[index] = total.astype(jnp.bfloat16)
                    else:
                        gs[pl.ds(SECTIONS[s] + first + row, n)] = total.astype(jnp.bfloat16).astype(jnp.float32)

                loop(near, add)

    flat[flat.shape[0] - 8 :] = jnp.zeros((8, LANES), jnp.float32)
    stages = [(what, k) for k in PHASES for what in (middle, finish)]

    def tick(time):
        for s in range(len(SECTIONS)):
            if 0 <= time - s < len(stages):
                what, k = stages[time - s]
                what(s, k)
                if what is finish and k < 2:
                    begin(s, k + 1)

    for s in range(len(SECTIONS)):
        products(s)
        if s == 0:
            pl.semaphore_wait(barrier, 9)
        begin(s, 0)
        tick(s - 1)
    arrive()
    for time in range(len(SECTIONS) - 1, len(SECTIONS) + len(stages) - 1):
        tick(time)

    part = jnp.zeros((1, LANES), jnp.float32)
    for row, rows, _ in PARTS.values():
        part += jnp.sum(gs[row : row + rows] * gs[row : row + rows], axis=0, keepdims=True)
    part = jnp.broadcast_to(part, (8, LANES))
    for copy in copies.values():
        copy.wait_send()
    sent = []
    for axis in PHASES:
        sq[axis, at[axis]] = part
        here = [push(sq.at[axis, at[axis]], sq.at[axis, at[axis]], "sq", (axis, by - 1), axis, by) for by in (1, 2, 3)]
        for copy in here:
            copy.start()
        for copy in here:
            copy.wait_recv()
        part = (sq[axis, 0] + sq[axis, 1]) + (sq[axis, 2] + sq[axis, 3])
        sent += here
    total = jnp.sum(part[0:1], axis=1, keepdims=True)
    factor = jnp.broadcast_to(jnp.minimum(1.0, 0.5 * lax.rsqrt(total / count + 1e-30)), (1, LANES))

    def rows_of(i):
        here = pl.ds(pl.multiple_of(i * 96, 32), 96)
        new, r["new_m"][here], r["new_v"][here] = adamw(r["own"][here], r["m"][here], r["v"][here], gs[here] * factor)
        grad[at[0], at[1], at[2], here] = new

    _repeat(FLAT // 96, rows_of)

    hops, outs = {}, []

    def piece(ref, c, k, by, half):
        known = {**{ORDERS[c][j]: at[ORDERS[c][j]] for j in range(k)}, ORDERS[c][k]: place(ORDERS[c][k], by)}
        return _blocks(ref, known, c * THIRD + (0 if half == "a" else THIRD // 2), THIRD // 2)

    def hop(c, k, i, by, half, to):
        hops[c, k, i] = push(piece(grad, c, k, by, half), piece(grad, c, k, by, half), "hop", (c, k, i), ORDERS[c][k], to)
        hops[c, k, i].start()

    def flush(c, by, half):
        copy = pltpu.make_async_copy(piece(grad, c, 0, by, half), piece(r["out"], c, 0, by, half), r["out_sem"].at[len(outs)])
        copy.start()
        outs.append(copy)

    def lead(c, k):
        for i, (half, to) in enumerate((("a", 1), ("b", -1), ("b", 1), ("a", -1))):
            hop(c, k, i, 0, half, to)

    for c in COLOURS:
        lead(c, 2)
    for k in reversed(PHASES):
        for c in COLOURS:
            hops[c, k, 0].wait_recv()
            hop(c, k, 4, -1, "a", 1)
            hops[c, k, 1].wait_recv()
            hop(c, k, 5, 1, "b", -1)
            if k == 0:
                for by, half in ((0, "a"), (0, "b"), (-1, "a"), (1, "b")):
                    flush(c, by, half)
        for c in COLOURS:
            for i, by, half in ((2, -1, "b"), (3, 1, "a"), (4, 2, "a"), (5, 2, "b")):
                hops[c, k, i].wait_recv()
                if k == 0:
                    flush(c, by, half)
            if k:
                lead(c, k - 1)
    for copy in outs:
        copy.wait()
    for copy in (*sent, *hops.values()):
        copy.wait_send()


def adamw(w, m, v, g):
    m = 0.9 * m + 0.1 * g
    v = 0.95 * v + 0.05 * g * g
    step = m * lax.rsqrt(v + 1e-8) + 0.1 * w
    return (w - 0.02 * step).astype(jnp.bfloat16), m, v


def tail(weights, m, v, **streams):
    low, f32, dma = jnp.bfloat16, jnp.float32, pltpu.SemaphoreType.DMA
    hbm, vmem = pl.BlockSpec(memory_space=pl.ANY), pl.BlockSpec(memory_space=pltpu.VMEM)
    count = float(64 * sum(one.size for one in m.values()))
    given = {**streams, **weights, **{(kind, name): one for kind, of in (("m", m), ("v", v)) for name, one in of.items()}}
    tokens = streams["a"].shape[0]
    sums, hops, squares = dma((4, 3, 3, 6)), dma((3, 3, 6)), dma((3, 3))
    scratch = {
        "grad": pltpu.VMEM((*CUBE, FLAT, LANES), low), "flat": pltpu.VMEM((64 * 250 + 8, LANES), f32), "gs": pltpu.VMEM((FLAT, LANES), f32),
        "sq": pltpu.VMEM((3, 4, 8, LANES), f32),
        "stream": pltpu.VMEM((2, tokens, TILE), low), "left": pltpu.VMEM((TILE, tokens), low), "right": pltpu.VMEM((tokens, TILE), low),
        "found": pltpu.VMEM((400, LANES), f32), "wo_m": pltpu.VMEM(m["wo"].shape, f32), "wo_v": pltpu.VMEM(m["wo"].shape, f32),
        "own_sem": dma((21,)), "spare": pltpu.VMEM((tokens, TILE), low), "stream_sem": dma((2,)), "fixed_sem": dma((2,)), "sum_send": sums, "sum_recv": sums,
        "hop_send": hops, "hop_recv": hops, "sq_send": squares, "sq_recv": squares, "out_sem": dma((24,)),
    }
    for name in ("own", "m", "v"):
        scratch[name] = pltpu.VMEM((FLAT, LANES), f32)
    for name, w in weights.items():
        scratch["near", name] = pltpu.VMEM((56 if name == "w_down" else 16, w.shape[1]), low)
    for s in range(len(SECTIONS)):
        for c in COLOURS:
            _, na, nb = CUTS[s][c]
            for k in PHASES:
                lead = CUBE[k + 1 :]
                for name in ("opp", "dir", "acc"):
                    scratch[name + "_a", s, c, k] = pltpu.VMEM((*lead, na, LANES), low)
                    scratch[name + "_b", s, c, k] = pltpu.VMEM((*lead, nb, LANES), low)
                if k < 2:
                    scratch["sum", s, c, k] = pltpu.VMEM((*lead, na + nb, LANES), f32)
    moment = jax.ShapeDtypeStruct((FLAT, LANES), f32)
    return pl.pallas_call(
        functools.partial(_tail, count, [*given, "out", "new_m", "new_v", *scratch]),
        in_specs=[hbm] * len(given),
        out_specs=[hbm, vmem, vmem],
        out_shape=[jax.ShapeDtypeStruct((*CUBE, FLAT, LANES), low), moment, moment],
        scratch_shapes=list(scratch.values()),
        compiler_params=pltpu.CompilerParams(collective_id=0, has_side_effects=True, vmem_limit_bytes=67_000_000),
    )(*given.values())


def _spread(flat_in, m_in, v_in, *refs):
    outs, (came, flat, wide, high, qkv, moment, in_sem, out_sem, moment_sem) = refs[:21], refs[21:]

    def fetch(i, row, rows):
        rows = -(-rows // 16) * 16
        return pltpu.make_async_copy(flat_in.at[:, :, :, pl.ds(row, rows)], came.at[i % 2, :, :, :, pl.ds(0, rows)], in_sem.at[i % 2])

    parts = list(PARTS.items())
    copies = []

    def give(src, dst, sem):
        copies.append(pltpu.make_async_copy(src, dst, sem))
        copies[-1].start()

    fetch(0, *parts[0][1][:2]).start()
    for i, (name, (row, per, tiles)) in enumerate(parts):
        for kind, ref in enumerate((m_in, v_in)):
            out = outs[7 * (kind + 1) + i]
            if name == "wo":
                for c in range(tiles):
                    moment[kind, :, _lanes(c)] = ref[pl.ds(row + c, out.shape[0], stride=tiles), :]
                give(moment.at[kind], out, moment_sem.at[kind, i])
            else:
                give(ref.at[pl.ds(row, per)], out.at[:, 0], moment_sem.at[kind, i])
    for i, (name, (row, per, tiles)) in enumerate(parts):
        if i + 1 < len(parts):
            fetch(i + 1, *parts[i + 1][1][:2]).start()
        fetch(i, row, per).wait()

        def four(q, i=i, per=per):
            base = pl.multiple_of(q * (4 * per), 8)
            for z in range(4):
                flat[pl.ds(base + per * z, per), :] = came[i % 2, *_xy(q), z, :per].astype(jnp.float32)

        _repeat(16, four)
        rows = outs[i].shape[0]
        first = {"wk": 8, "wv": 9}.get(name, 0)
        buf = {"w_gate": wide.at[0], "w_up": wide.at[1], "w_down": high.at[0], "wo": high.at[1, :rows]}.get(name, qkv)
        step = TILE if rows % TILE == 0 else 512

        def gather(j, buf=buf, tiles=tiles, step=step, first=first):
            at = pl.multiple_of(j * step, step)
            for c in range(tiles):
                buf[pl.ds(at, step), _lanes(first + c)] = flat[pl.ds(at * tiles + c, step, stride=tiles), :].astype(jnp.bfloat16)

        _repeat(rows // step, gather)
        give(buf.at[:, _lanes(first, tiles)], outs[i], out_sem.at[i])
    for copy in copies:
        copy.wait()


def spread(flat, new_m, new_v, weights, m):
    low, f32, dma = jnp.bfloat16, jnp.float32, pltpu.SemaphoreType.DMA
    hbm, vmem = pl.BlockSpec(memory_space=pl.ANY), pl.BlockSpec(memory_space=pltpu.VMEM)
    shapes = [jax.ShapeDtypeStruct(weights[n].shape, low) for n in PARTS] + [jax.ShapeDtypeStruct(m[n].shape, f32) for n in PARTS] * 2
    d, units = weights["w_gate"].shape
    return pl.pallas_call(
        _spread,
        in_specs=[hbm, vmem, vmem],
        out_specs=[hbm] * len(shapes),
        out_shape=shapes,
        scratch_shapes=[pltpu.VMEM((2, *CUBE, 256, LANES), low), pltpu.VMEM((64 * 250, LANES), f32), pltpu.VMEM((2, d, units), low),
                        pltpu.VMEM((2, units, d), low), pltpu.VMEM((d, 2 * TILE), low), pltpu.VMEM((2, *m["wo"].shape), f32),
                        dma((2,)), dma((7,)), dma((2, 7))],
        compiler_params=pltpu.CompilerParams(vmem_limit_bytes=64_000_000),
    )(flat, new_m, new_v)


def solution(mesh):
    def step(x, dy, *arrays):
        w, m, v = (dict(zip(NAMES, (one[0] for one in arrays[i : i + 7]))) for i in (0, 7, 14))
        x, dy = x[0], dy[0]
        a, q, k, val, cos, sin, h, b, att, lse = front(x, w["wq"], w["wk"], w["wv"], w["wo"])
        act, by_gate, by_up, by_h, by_att = ffn(b, h, dy, w["w_gate"], w["w_up"], w["w_down"], w["wo"])
        by_qkv = attend_bwd(q, k, val, cos, sin, by_att, att, lse)

        lined = lambda of: {n: one if n == "wo" else one.reshape(-1, 1, LANES) for n, one in of.items()}
        m_lined = lined(m)
        flat = tail({n: w[n] for n in PARTS}, m_lined, lined(v), a=a, b=b, act=act, att=att, dy=dy, by_h=by_h, by_gate=by_gate, by_up=by_up, by_qkv=by_qkv)
        outs = spread(*flat, w, m_lined)
        new = [dict(zip(PARTS, outs[i : i + 7])) for i in (0, 7, 14)]
        return tuple(one[n].reshape(1, *like[n].shape) for one, like in zip(new, (w, m, m)) for n in NAMES)

    states, all_of, cut = P(("rep", "dp")), P(), P(None, "dp")
    return jax.shard_map(
        step,
        mesh=mesh,
        in_specs=(states, states) + (all_of,) * 7 + (cut,) * 14,
        out_specs=(P("rep"),) * 7 + (P("rep", "dp"),) * 14,
        check_vma=False,
    )
```

```python
import functools

import jax
import jax.numpy as jnp
import numpy as np
from jax import lax
from jax.experimental import pallas as pl
from jax.experimental.pallas import tpu as pltpu
from jax.sharding import PartitionSpec as P


NEG = -1e30
HIDDEN = 2 * NEG
LOG2E = 1.4426950408889634
VMEM = 56 * 2**20
STRIP = 512
CHUNK = 256
WIDE = 1280
ALL = ...
HEAD = LANES = 128
HEADS = 8
TILE = 640
SCALE = HEAD**-0.5
THETA = 10000
NAMES = ("wq", "wk", "wv", "wo", "w_gate", "w_up", "w_down")


NN, NT = (1, 0), (1, 1)


def _dot(a, b, ca, cb):
    return lax.dot_general(a, b, (((ca,), (cb,)), ((), ())), preferred_element_type=jnp.float32)


def _repeat(last, body, first=0):
    lax.fori_loop(first, last, lambda i, _: body(i), None)


def _lanes(n, tiles=1):
    return slice(n * LANES, (n + tiles) * LANES)


def _gap(bk, cols, bq):
    return lax.rem(lax.broadcasted_iota(jnp.int32, (bk, cols), 1), bq) - lax.broadcasted_iota(jnp.int32, (bk, cols), 0)


def _heads(ref):
    return [ref[:, _lanes(n)] for n in range(ref.shape[1] // HEAD)]


def _stacked(ref):
    return jnp.concatenate(_heads(ref), axis=0)


def _turned(t, cos, sin):
    t = t.astype(jnp.float32)
    return (t * cos + pltpu.roll(t, HEAD // 2, 1) * sin).astype(jnp.bfloat16)


def _setup(k, cos_ref, sin_ref, gap_s, k_s, bq, bk):
    gap_s[ALL] = _gap(bk, HEADS * bq, bq)
    k_s[ALL] = _turned(k, cos_ref[ALL], sin_ref[ALL])


def _queries(q, cos_ref, sin_ref, q_s, bq):
    here = pl.ds(pl.multiple_of(pl.program_id(0) * bq, bq), bq)
    cos, sin = cos_ref[here, :], sin_ref[here, :]
    for n, t in enumerate(_heads(q)):
        q_s[n * bq : (n + 1) * bq, :] = _turned(t, cos, sin)
    return cos, sin, here


def _normed(h):
    wide = h.astype(jnp.float32)
    scale = lax.rsqrt(jnp.mean(wide * wide, -1, keepdims=True) + 1e-6)
    return wide, scale


def _front(x_ref, wq_ref, wk_ref, wv_ref, wo_ref, few_ref, a_ref, q_ref, k_ref, v_ref, cos_ref, sin_ref, h_ref, b_ref, o_ref, lse_ref,
           top_s, mix_s, gap_s, q_s, k_s, *, bq, bk):
    cols, iq, e, low = HEADS * bq, pl.program_id(0), SCALE * LOG2E, x_ref.dtype
    pieces = range(0, cols, STRIP)

    @pl.when(iq == 0)
    def _():
        few = few_ref.shape[1]
        for n in range(a_ref.shape[0] // few):
            cos, sin = few_ref[0, n : n + 1], few_ref[1, n : n + 1]
            cos_ref[n * few : (n + 1) * few, :] = cos * few_ref[2] - sin * few_ref[3]
            sin_ref[n * few : (n + 1) * few, :] = sin * few_ref[2] + cos * few_ref[3]
        half = lax.broadcasted_iota(jnp.int32, sin_ref.shape, 1) < HEAD // 2
        sin_ref[ALL] = jnp.where(half, -sin_ref[ALL], sin_ref[ALL])
        wide, scale = _normed(x_ref[ALL])
        a_ref[ALL] = (wide * scale).astype(low)
        k = _dot(a_ref[ALL], wk_ref[ALL], *NN).astype(low)
        k_ref[ALL] = k
        v_ref[ALL] = _dot(a_ref[ALL], wv_ref[ALL], *NN).astype(low)
        _setup(k, cos_ref, sin_ref, gap_s, k_s, bq, bk)

    rows = pl.ds(pl.multiple_of(iq * bq, bq), bq)
    q_ref[ALL] = _dot(a_ref[rows, :], wq_ref[ALL], *NN).astype(low)
    _queries(q_ref, cos_ref, sin_ref, q_s, bq)
    top_s[ALL] = jnp.full(top_s.shape, NEG, jnp.float32)
    mix_s[ALL] = jnp.zeros_like(mix_s)
    ones = jnp.ones((8, bk), k_ref.dtype)

    def block(j, masked):
        here = pl.ds(j * bk, bk)
        scores = [_dot(k_s[here, :], q_s[at : at + STRIP, :], *NT) for at in pieces]
        weights, keeps = [], []
        for at, s in zip(pieces, scores):
            if masked:
                s = jnp.where(gap_s[:, at : at + STRIP] >= j * bk - iq * bq, s, HIDDEN)
            old = top_s[:, at : at + STRIP]
            top = jnp.maximum(old, s.max(axis=0, keepdims=True))
            top_s[:, at : at + STRIP] = top
            weights.append(jnp.exp2((s - top) * e).astype(v_ref.dtype))
            keeps.append(jnp.exp2((old - top) * e))
        values = jnp.concatenate([v_ref[here, :].T, ones], axis=0)
        for at, p, keep in zip(pieces, weights, keeps):
            mix_s[:, at : at + STRIP] = mix_s[:, at : at + STRIP] * keep + _dot(values, p, *NN)

    whole = iq * (bq // bk)
    _repeat(whole, lambda j: block(j, False))
    _repeat(whole + bq // bk, lambda j: block(j, True), whole)
    total = mix_s[HEAD : HEAD + 1, :]
    mix = (mix_s[:HEAD, :] * (1 / total)).T.astype(o_ref.dtype)
    lse = top_s[ALL] * SCALE + jnp.log(total)
    for n in range(HEADS):
        o_ref[:, _lanes(n)] = mix[n * bq : (n + 1) * bq]
        lse_ref[n : n + 1, :] = lse[:, n * bq : (n + 1) * bq]
    h = x_ref[rows, :] + _dot(o_ref[ALL], wo_ref[ALL], *NN).astype(low)
    h_ref[ALL] = h
    wide, scale = _normed(h)
    b_ref[ALL] = (wide * scale).astype(low)


def _backward(q_ref, k_ref, v_ref, cos_ref, sin_ref, do_ref, o_ref, lse_ref, by_ref, dq_s, dk_s, dv_s, gap_s, q_s, k_s, do_s, *, bq, bk):
    cols, iq, e, low = HEADS * bq, pl.program_id(0), SCALE * LOG2E, q_ref.dtype
    pieces = range(0, cols, STRIP)
    cos, sin, rows = _queries(q_ref, cos_ref, sin_ref, q_s, bq)

    @pl.when(iq == 0)
    def _():
        _setup(k_ref[ALL], cos_ref, sin_ref, gap_s, k_s, bq, bk)
        dk_s[ALL] = jnp.zeros_like(dk_s)
        dv_s[ALL] = jnp.zeros_like(dv_s)

    dq_s[ALL] = jnp.zeros_like(dq_s)
    do_s[ALL] = _stacked(do_ref)
    lses = jnp.concatenate([lse_ref[n : n + 1, :] for n in range(HEADS)], axis=1) * LOG2E
    both = do_s[ALL].astype(jnp.float32) * _stacked(o_ref).astype(jnp.float32)
    deltas = both.T.sum(axis=0, keepdims=True)

    def block(j, masked):
        here = pl.ds(j * bk, bk)
        qs = [q_s[at : at + STRIP, :] for at in pieces]
        dos = [do_s[at : at + STRIP, :] for at in pieces]
        scores = [_dot(k_s[here, :], x, *NT) for x in qs]
        dps = [_dot(v_ref[here, :], x, *NT) for x in dos]
        for n, at in enumerate(pieces):
            p = jnp.exp2(scores[n] * e - lses[:, at : at + STRIP])
            if masked:
                p = jnp.where(gap_s[:, at : at + STRIP] >= j * bk - iq * bq, p, 0.0)
            ds = (p * (dps[n] - deltas[:, at : at + STRIP])).astype(low)
            dv_s[here, :] += _dot(p.astype(low), dos[n], *NN)
            dk_s[here, :] += _dot(ds, qs[n], *NN)
            dq_s[:, at : at + STRIP] += _dot(k_s[here, :].T, ds, *NN)

    whole = iq * (bq // bk)
    _repeat(whole, lambda j: block(j, False))
    _repeat(whole + bq // bk, lambda j: block(j, True), whole)
    dq, cols_q = (dq_s[ALL] * SCALE).T.astype(low), HEADS * HEAD
    for n in range(HEADS):
        by_ref[rows, _lanes(n)] = _turned(dq[n * bq : (n + 1) * bq], cos, -sin)

    @pl.when(iq == pl.num_programs(0) - 1)
    def _():
        by_ref[:, cols_q : cols_q + HEAD] = _turned((dk_s[ALL] * SCALE).astype(low), cos_ref[ALL], -sin_ref[ALL])
        by_ref[:, cols_q + HEAD :] = dv_s[ALL].astype(low)


def _attention_call(kernel, bq, bk, given, results, scratch):
    def spec(shape, cut):
        if cut is None:
            return pl.BlockSpec(shape, lambda i: (0,) * len(shape))
        return pl.BlockSpec((bq, shape[1]), lambda i: (i, 0)) if cut == 0 else pl.BlockSpec((shape[0], bq), lambda i: (0, i))

    tokens = given[0][0].shape[0]
    return pl.pallas_call(
        functools.partial(kernel, bq=bq, bk=bk),
        grid=(tokens // bq,),
        in_specs=[spec(a.shape, cut) for a, cut in given],
        out_specs=[spec(a.shape, cut) for a, cut in results],
        out_shape=[a for a, _ in results],
        scratch_shapes=scratch,
        compiler_params=pltpu.CompilerParams(dimension_semantics=("arbitrary",), vmem_limit_bytes=VMEM),
    )(*[a for a, _ in given])


def angles(tokens):
    few = int(tokens**0.5)
    turn = np.tile(THETA ** (-np.arange(HEAD // 2) / (HEAD // 2)), 2)
    far, near = (np.arange(few)[:, None] * turn * by for by in (few, 1))
    return np.stack([np.cos(far), np.sin(far), np.cos(near), np.sin(near)]).astype(np.float32)


def front(x, wq, wk, wv, wo):
    bq, bk = 512, 256
    tokens, d = x.shape
    cols, f32 = HEADS * bq, jnp.float32
    like = lambda n, t=x.dtype: jax.ShapeDtypeStruct((tokens, n), t)
    return _attention_call(
        _front, bq, bk, [(one, None) for one in (x, wq, wk, wv, wo, angles(tokens))],
        [(like(d), None), (like(wq.shape[1]), 0), (like(HEAD), None), (like(HEAD), None), (like(HEAD, f32), None), (like(HEAD, f32), None),
         (like(d), 0), (like(d), 0), (like(wo.shape[0]), 0), (jax.ShapeDtypeStruct((HEADS, tokens), f32), 1)],
        [pltpu.VMEM((1, cols), f32), pltpu.VMEM((HEAD + 8, cols), f32), pltpu.VMEM((bk, cols), jnp.int32), pltpu.VMEM((cols, HEAD), x.dtype),
         pltpu.VMEM((tokens, HEAD), x.dtype)])


def attend_bwd(q, k, v, cos, sin, d_out, out, lse):
    bq = bk = 256
    cols, like = HEADS * bq, jax.ShapeDtypeStruct
    f32 = jnp.float32
    return _attention_call(
        _backward, bq, bk, [(q, 0), (k, None), (v, None), (cos, None), (sin, None), (d_out, 0), (out, 0), (lse, 1)],
        [(like((q.shape[0], q.shape[1] + 2 * HEAD), q.dtype), None)],
        [pltpu.VMEM((HEAD, cols), f32), pltpu.VMEM(k.shape, f32), pltpu.VMEM(k.shape, f32), pltpu.VMEM((bk, cols), jnp.int32),
         pltpu.VMEM((cols, HEAD), q.dtype), pltpu.VMEM(k.shape, k.dtype), pltpu.VMEM((cols, HEAD), q.dtype)])[0]


def _ffn(b_ref, h_ref, dy_ref, wg_hbm, wu_hbm, wd_hbm, wo_ref, act_ref, dg_ref, du_ref, dh_ref, do_ref, wg, wu, wd, acc_g, acc_u, sems):
    low, units, first = act_ref.dtype, wg.shape[1], pl.program_id(0) == 0
    coming = [pltpu.make_async_copy(src, dst, sems.at[n]) for n, (src, dst) in enumerate(((wg_hbm, wg), (wu_hbm, wu), (wd_hbm, wd)))]

    def at_first(what):
        @pl.when(first)
        def _():
            what()

    def settle(n):
        at_first(coming[n].wait)

    at_first(lambda: [copy.start() for copy in coming])
    for at in range(0, units, WIDE):
        here = slice(at, min(at + WIDE, units))
        if at == 0:
            settle(0)
        gate = _dot(b_ref[ALL], wg[:, here], *NN)
        if at == 0:
            settle(1)
        up = _dot(b_ref[ALL], wu[:, here], *NN)
        if at == 0:
            settle(2)
        d = _dot(dy_ref[ALL], wd[here, :], *NT).astype(low).astype(jnp.float32)
        s = jax.nn.sigmoid(gate)
        silu = gate * s
        act_ref[:, here] = (silu * up).astype(low)
        du, dg = (d * silu).astype(low), (d * up * (s * (1 + gate * (1 - s)))).astype(low)
        du_ref[:, here], dg_ref[:, here] = du, dg
        by_g, by_u = _dot(dg, wg[:, here], *NT), _dot(du, wu[:, here], *NT)
        if at == 0:
            acc_g[ALL], acc_u[ALL] = by_g, by_u
        else:
            acc_g[ALL] += by_g
            acc_u[ALL] += by_u
    d = (acc_g[ALL].astype(low) + acc_u[ALL].astype(low)).astype(jnp.float32)
    wide, scale = _normed(h_ref[ALL])
    along = jnp.mean(d * wide, -1, keepdims=True) * (scale * scale * scale)
    dh_ref[ALL] = dy_ref[ALL] + (d * scale - wide * along).astype(low)
    do_ref[ALL] = _dot(dh_ref[ALL], wo_ref[ALL], *NT).astype(low)


def ffn(b, h, dy, w_gate, w_up, w_down, wo):
    tokens, d = b.shape
    units = w_gate.shape[1]
    rows = lambda n: pl.BlockSpec((CHUNK, n), lambda i: (i, 0))
    like = lambda n: jax.ShapeDtypeStruct((tokens, n), b.dtype)
    widths = [units] * 3 + [d, wo.shape[0]]
    return pl.pallas_call(
        _ffn,
        grid=(tokens // CHUNK,),
        in_specs=[rows(d)] * 3 + [pl.BlockSpec(memory_space=pl.ANY)] * 3 + [pl.BlockSpec(wo.shape, lambda i: (0, 0))],
        out_specs=[rows(n) for n in widths],
        out_shape=[like(n) for n in widths],
        scratch_shapes=[*(pltpu.VMEM(w.shape, w.dtype) for w in (w_gate, w_up, w_down)), *[pltpu.VMEM((CHUNK, d), jnp.float32)] * 2,
                        pltpu.SemaphoreType.DMA((3,))],
        compiler_params=pltpu.CompilerParams(dimension_semantics=("arbitrary",), vmem_limit_bytes=62_000_000),
    )(b, h, dy, w_gate, w_up, w_down, wo)


CUBE = (4, 4, 4)
AXES = (16, 4, 1)
ORDERS = ((0, 1, 2), (1, 2, 0), (2, 0, 1))
PHASES = COLOURS = (0, 1, 2)
SECTIONS = (0, 256, 512, 768)
FLAT = 960
SMALL = ((0, 32, 32), (64, 32, 32), (128, 32, 32))
BIG = ((0, 48, 48), (96, 48, 32), (176, 32, 48))
CUTS = (BIG, (BIG[2], BIG[0], BIG[1]), (BIG[1], BIG[2], BIG[0]), SMALL)
THIRD = FLAT // 3
PARTS = {"w_gate": (0, 250, 25), "w_up": (256, 250, 25), "w_down": (512, 250, 5), "wq": (768, 80, 8), "wk": (848, 10, 1), "wv": (864, 10, 1), "wo": (880, 80, 5)}
KEYS = 640 * 8
MESH = pl.DeviceIdType.MESH


def _where():
    me = lax.axis_index("dp")
    return me, (lax.div(me, AXES[0]), *_xy(lax.rem(me, 16)))


def _xy(q):
    return lax.div(q, 4), lax.rem(q, 4)


def _blocks(ref, fixed, row, n):
    index = [slice(None)] * 3
    for axis, i in fixed.items():
        index[axis] = i
    return ref.at[(*index, pl.ds(row, n))]


def _tail(count, names, *refs):
    r = dict(zip(names, refs))
    grad, flat, gs, sq = (r[n] for n in ("grad", "flat", "gs", "sq"))
    me, at = _where()

    def place(axis, by):
        return lax.rem(at[axis] + (by + 4), 4)

    def peer(axis, by):
        return {"dp": me + (place(axis, by) - at[axis]) * AXES[axis]}

    def push(src, dst, sems, index, axis, by):
        return pltpu.make_async_remote_copy(src_ref=src, dst_ref=dst, send_sem=r[sems + "_send"].at[index], recv_sem=r[sems + "_recv"].at[index],
                                            device_id=peer(axis, by), device_id_type=MESH)

    barrier = pltpu.get_barrier_semaphore()
    for axis in PHASES:
        for by in (1, 2, 3):
            pl.semaphore_signal(barrier, inc=1, device_id=peer(axis, by), device_id_type=MESH)

    moves = []

    def move(src, dst):
        moves.append(pltpu.make_async_copy(src, dst, r["own_sem"].at[len(moves)]))
        moves[-1].start()

    shift = {}
    for name, (row, rows, tiles) in PARTS.items():
        own_rows = rows // tiles
        first = lax.div(me * own_rows, 8) * 8
        shift[name] = me * own_rows - first
        near = r["near", name]
        move(r[name].at[pl.ds(pl.multiple_of(first, 8), near.shape[0])], near)
        for kind in "mv":
            given = r[kind, name]
            move(given, r["wo_" + kind]) if name == "wo" else move(given.at[:, 0], r[kind].at[pl.ds(row, rows)])

    def arrive():
        for copy in moves:
            copy.wait()
        for name, (row, rows, tiles) in PARTS.items():
            near, found = r["near", name], r["found"]
            for c in range(tiles):
                lanes = _lanes(c)
                found[pl.ds(c, near.shape[0], stride=tiles), :] = near[:, lanes].astype(jnp.float32)
                if name == "wo":
                    for kind in "mv":
                        r[kind][pl.ds(row + c, near.shape[0], stride=tiles), :] = r["wo_" + kind][:, lanes]
            r["own"][row : row + rows] = found[pl.ds(shift[name] * tiles, rows), :]

    stream, left, right, spare = r["stream"], r["left"], r["right"], r["spare"]
    JOBS = (("by_gate", 5, TILE), ("by_up", 5, TILE), ("act", 5, TILE), ("by_qkv", 2, TILE), ("att", 2, 512))

    def load(i, j, slot):
        name, _, width = JOBS[i]
        return pltpu.make_async_copy(r[name].at[:, pl.ds(j * width, width)], stream.at[slot, :, pl.ds(0, width)], r["stream_sem"].at[slot])

    def fetch(name, target, sem):
        copy = pltpu.make_async_copy(r[name], target, r["fixed_sem"].at[sem])
        copy.start()
        return copy

    def each(i, use):
        number, before = JOBS[i][1], sum(n for _, n, _ in JOBS[:i])

        def step(j):
            slot = lax.rem(before + j, 2)

            @pl.when(j + 1 < number)
            def _():
                load(i, j + 1, 1 - slot).start()

            if i + 1 < len(JOBS):
                @pl.when(j + 1 == number)
                def _():
                    load(i + 1, 0, 1 - slot).start()

            load(i, j, slot).wait()
            use(j, stream[slot, :, : JOBS[i][2]])

        _repeat(number, step)

    def job(i, keep_left, tiles):
        width = JOBS[i][2]

        def use(j, tile):
            if keep_left:
                out, base = _dot(left[ALL], tile, *NN), j * (width // LANES)
            else:
                out, base = _dot(tile.T, right[ALL], *NN), j * (width * tiles)
            for c in range(out.shape[1] // LANES):
                flat[pl.ds(base + c, out.shape[0], stride=tiles), :] = out[:, _lanes(c)]

        each(i, use)

    def pack(name, start=0):
        row, per, _ = PARTS[name]
        rows = -(-per // 16) * 16

        def four(q):
            base = pl.multiple_of(start + q * (4 * per), 8)
            for z in range(4):
                grad[*_xy(q), z, row : row + rows] = flat[pl.ds(base + per * z, rows), :].astype(jnp.bfloat16)

        _repeat(16, four)

    coming = [fetch("b", spare, 0), fetch("dy", right, 1)]
    load(0, 0, 0).start()

    def products(s):
        if s < 2:
            if s == 0:
                coming[0].wait()
                left[ALL] = spare[ALL].T
                coming.append(fetch("a", spare, 0))
            job(s, True, 25)
            pack(("w_gate", "w_up")[s])
        elif s == 2:
            coming[1].wait()
            job(s, False, 5)
            coming.append(fetch("by_h", right, 1))
            pack("w_down")
        else:
            coming[2].wait()
            left[ALL] = spare[ALL].T

            def use(j, tile):
                out = _dot(left[ALL], tile, *NN)
                for c in range(3):
                    flat[pl.ds(5 * j + c, TILE, stride=8), :] = out[:, _lanes(c)]
                for c in (3, 4):
                    @pl.when(j == 0)
                    def _(c=c):
                        flat[pl.ds(c, TILE, stride=8), :] = out[:, _lanes(c)]

                    @pl.when(j > 0)
                    def _(c=c):
                        flat[pl.ds(KEYS + (c - 3) * TILE, TILE), :] = out[:, _lanes(c)]

            each(s, use)
            pack("wq")
            pack("wk", KEYS)
            pack("wv", KEYS + TILE)
            coming[3].wait()
            job(s + 1, False, 5)
            pack("wo")

    def term(s, c, k, by, row, n):
        known = {ORDERS[c][j]: at[ORDERS[c][j]] for j in range(k)}
        return _blocks(grad, {**known, ORDERS[c][k]: place(ORDERS[c][k], by)}, SECTIONS[s] + CUTS[s][c][0] + row, n)

    def exact(s, c, k, by, row, n):
        if k == 0:
            return term(s, c, k, by, row, n)
        i, here, ref = place(ORDERS[c][k], by), pl.ds(row, n), r["sum", s, c, k - 1]
        if k == 1 and ORDERS[c][1] > ORDERS[c][2]:
            return ref.at[:, i, here]
        return ref.at[i, :, here] if k == 1 else ref.at[i, here]

    def loop(ref, body):
        if len(ref.shape) > 3:
            _repeat(ref.shape[0], lambda i: body((i,)))
        else:
            body(())

    copies = {}
    wide = lambda ref, index: ref[index].astype(jnp.float32)

    def send(s, c, k, name, i, src, to):
        copy = push(src, r[name, s, c, k], "sum", (s, c, k, i), ORDERS[c][k], to)
        copy.start()
        copies[s, c, k, name] = copy

    def begin(s, k):
        for c in COLOURS:
            _, na, nb = CUTS[s][c]
            for i, (name, by, row, n, to) in enumerate((("opp_a", 2, 0, na, 1), ("opp_b", 2, na, nb, -1), ("dir_b", 1, na, nb, 1), ("dir_a", -1, 0, na, -1))):
                send(s, c, k, name, i, term(s, c, k, by, row, n), to)

    def middle(s, k):
        for c in COLOURS:
            _, na, nb = CUTS[s][c]
            for i, (half, by, row, n) in enumerate((("a", 1, 0, na), ("b", -1, na, nb))):
                copies[s, c, k, "opp_" + half].wait_recv()
                came, mine, to = r["opp_" + half, s, c, k], exact(s, c, k, by, row, n), term(s, c, k, by, row, n)

                def add(index, came=came, mine=mine, to=to):
                    to[index] = (wide(mine, index) + wide(came, index)).astype(jnp.bfloat16)

                loop(came, add)
                send(s, c, k, "acc_" + half, 4 + i, to, by)

    def finish(s, k):
        for c in COLOURS:
            first, na, nb = CUTS[s][c]
            for half, row, n in (("a", 0, na), ("b", na, nb)):
                copies[s, c, k, "dir_" + half].wait_recv()
                copies[s, c, k, "acc_" + half].wait_recv()
                near, far, mine, low = r["dir_" + half, s, c, k], r["acc_" + half, s, c, k], exact(s, c, k, 0, row, n), term(s, c, k, 0, row, n)

                def add(index, near=near, far=far, mine=mine, low=low, row=row, n=n, c=c, first=first):
                    total = wide(mine, index) + (wide(near, index) + wide(far, index))
                    if k < 2:
                        r["sum", s, c, k].at[(slice(None),) * (2 - k) + (pl.ds(row, n),)][index] = total
                        low[index] = total.astype(jnp.bfloat16)
                    else:
                        gs[pl.ds(SECTIONS[s] + first + row, n)] = total.astype(jnp.bfloat16).astype(jnp.float32)

                loop(near, add)

    flat[flat.shape[0] - 8 :] = jnp.zeros((8, LANES), jnp.float32)
    stages = [(what, k) for k in PHASES for what in (middle, finish)]

    def tick(time):
        for s in reversed(range(len(SECTIONS))):
            if 0 <= time - s < len(stages):
                what, k = stages[time - s]
                what(s, k)
                if what is finish and k < 2:
                    begin(s, k + 1)

    for s in range(len(SECTIONS)):
        products(s)
        if s == 0:
            pl.semaphore_wait(barrier, 9)
        begin(s, 0)
        tick(s - 1)
    arrive()
    for time in range(len(SECTIONS) - 1, len(SECTIONS) + len(stages) - 1):
        tick(time)

    part = jnp.zeros((1, LANES), jnp.float32)
    for row, rows, _ in PARTS.values():
        part += jnp.sum(gs[row : row + rows] * gs[row : row + rows], axis=0, keepdims=True)
    part = jnp.broadcast_to(part, (8, LANES))
    for copy in copies.values():
        copy.wait_send()
    sent = []
    for axis in PHASES:
        sq[axis, at[axis]] = part
        here = [push(sq.at[axis, at[axis]], sq.at[axis, at[axis]], "sq", (axis, by - 1), axis, by) for by in (1, 2, 3)]
        for copy in here:
            copy.start()
        for copy in here:
            copy.wait_recv()
        part = (sq[axis, 0] + sq[axis, 1]) + (sq[axis, 2] + sq[axis, 3])
        sent += here
    total = jnp.sum(part[0:1], axis=1, keepdims=True)
    factor = jnp.broadcast_to(jnp.minimum(1.0, 0.5 * lax.rsqrt(total / count + 1e-30)), (1, LANES))

    def rows_of(i):
        here = pl.ds(pl.multiple_of(i * 96, 32), 96)
        new, r["new_m"][here], r["new_v"][here] = adamw(r["own"][here], r["m"][here], r["v"][here], gs[here] * factor)
        grad[at[0], at[1], at[2], here] = new

    _repeat(FLAT // 96, rows_of)

    hops, outs = {}, []

    def piece(ref, c, k, by, half):
        known = {**{ORDERS[c][j]: at[ORDERS[c][j]] for j in range(k)}, ORDERS[c][k]: place(ORDERS[c][k], by)}
        return _blocks(ref, known, c * THIRD + (0 if half == "a" else THIRD // 2), THIRD // 2)

    def hop(c, k, i, by, half, to):
        hops[c, k, i] = push(piece(grad, c, k, by, half), piece(grad, c, k, by, half), "hop", (c, k, i), ORDERS[c][k], to)
        hops[c, k, i].start()

    def flush(c, by, half):
        copy = pltpu.make_async_copy(piece(grad, c, 0, by, half), piece(r["out"], c, 0, by, half), r["out_sem"].at[len(outs)])
        copy.start()
        outs.append(copy)

    def lead(c, k):
        for i, (half, to) in enumerate((("a", 1), ("b", -1), ("b", 1), ("a", -1))):
            hop(c, k, i, 0, half, to)

    for c in COLOURS:
        lead(c, 2)
    for k in reversed(PHASES):
        for c in COLOURS:
            hops[c, k, 0].wait_recv()
            hop(c, k, 4, -1, "a", 1)
            hops[c, k, 1].wait_recv()
            hop(c, k, 5, 1, "b", -1)
            if k == 0:
                for by, half in ((0, "a"), (0, "b"), (-1, "a"), (1, "b")):
                    flush(c, by, half)
        for c in COLOURS:
            for i, by, half in ((2, -1, "b"), (3, 1, "a"), (4, 2, "a"), (5, 2, "b")):
                hops[c, k, i].wait_recv()
                if k == 0:
                    flush(c, by, half)
            if k:
                lead(c, k - 1)
    for copy in outs:
        copy.wait()
    for copy in (*sent, *hops.values()):
        copy.wait_send()


def adamw(w, m, v, g):
    m = 0.9 * m + 0.1 * g
    v = 0.95 * v + 0.05 * g * g
    step = m * lax.rsqrt(v + 1e-8) + 0.1 * w
    return (w - 0.02 * step).astype(jnp.bfloat16), m, v


def tail(weights, m, v, **streams):
    low, f32, dma = jnp.bfloat16, jnp.float32, pltpu.SemaphoreType.DMA
    hbm, vmem = pl.BlockSpec(memory_space=pl.ANY), pl.BlockSpec(memory_space=pltpu.VMEM)
    count = float(64 * sum(one.size for one in m.values()))
    given = {**streams, **weights, **{(kind, name): one for kind, of in (("m", m), ("v", v)) for name, one in of.items()}}
    tokens = streams["a"].shape[0]
    sums, hops, squares = dma((4, 3, 3, 6)), dma((3, 3, 6)), dma((3, 3))
    scratch = {
        "grad": pltpu.VMEM((*CUBE, FLAT, LANES), low), "flat": pltpu.VMEM((64 * 250 + 8, LANES), f32), "gs": pltpu.VMEM((FLAT, LANES), f32),
        "sq": pltpu.VMEM((3, 4, 8, LANES), f32),
        "stream": pltpu.VMEM((2, tokens, TILE), low), "left": pltpu.VMEM((TILE, tokens), low), "right": pltpu.VMEM((tokens, TILE), low),
        "found": pltpu.VMEM((400, LANES), f32), "wo_m": pltpu.VMEM(m["wo"].shape, f32), "wo_v": pltpu.VMEM(m["wo"].shape, f32),
        "own_sem": dma((21,)), "spare": pltpu.VMEM((tokens, TILE), low), "stream_sem": dma((2,)), "fixed_sem": dma((2,)), "sum_send": sums, "sum_recv": sums,
        "hop_send": hops, "hop_recv": hops, "sq_send": squares, "sq_recv": squares, "out_sem": dma((24,)),
    }
    for name in ("own", "m", "v"):
        scratch[name] = pltpu.VMEM((FLAT, LANES), f32)
    for name, w in weights.items():
        scratch["near", name] = pltpu.VMEM((56 if name == "w_down" else 16, w.shape[1]), low)
    for s in range(len(SECTIONS)):
        for c in COLOURS:
            _, na, nb = CUTS[s][c]
            for k in PHASES:
                lead = CUBE[k + 1 :]
                for name in ("opp", "dir", "acc"):
                    scratch[name + "_a", s, c, k] = pltpu.VMEM((*lead, na, LANES), low)
                    scratch[name + "_b", s, c, k] = pltpu.VMEM((*lead, nb, LANES), low)
                if k < 2:
                    scratch["sum", s, c, k] = pltpu.VMEM((*lead, na + nb, LANES), f32)
    moment = jax.ShapeDtypeStruct((FLAT, LANES), f32)
    return pl.pallas_call(
        functools.partial(_tail, count, [*given, "out", "new_m", "new_v", *scratch]),
        in_specs=[hbm] * len(given),
        out_specs=[hbm, vmem, vmem],
        out_shape=[jax.ShapeDtypeStruct((*CUBE, FLAT, LANES), low), moment, moment],
        scratch_shapes=list(scratch.values()),
        compiler_params=pltpu.CompilerParams(collective_id=0, has_side_effects=True, vmem_limit_bytes=67_000_000),
    )(*given.values())


def _spread(flat_in, m_in, v_in, *refs):
    outs, (came, flat, wide, high, qkv, moment, in_sem, out_sem, moment_sem) = refs[:21], refs[21:]

    def fetch(i, row, rows):
        rows = -(-rows // 16) * 16
        return pltpu.make_async_copy(flat_in.at[:, :, :, pl.ds(row, rows)], came.at[i % 2, :, :, :, pl.ds(0, rows)], in_sem.at[i % 2])

    parts = list(PARTS.items())
    copies = []

    def give(src, dst, sem):
        copies.append(pltpu.make_async_copy(src, dst, sem))
        copies[-1].start()

    fetch(0, *parts[0][1][:2]).start()
    for i, (name, (row, per, tiles)) in enumerate(parts):
        for kind, ref in enumerate((m_in, v_in)):
            out = outs[7 * (kind + 1) + i]
            if name == "wo":
                for c in range(tiles):
                    moment[kind, :, _lanes(c)] = ref[pl.ds(row + c, out.shape[0], stride=tiles), :]
                give(moment.at[kind], out, moment_sem.at[kind, i])
            else:
                give(ref.at[pl.ds(row, per)], out.at[:, 0], moment_sem.at[kind, i])
    for i, (name, (row, per, tiles)) in enumerate(parts):
        if i + 1 < len(parts):
            fetch(i + 1, *parts[i + 1][1][:2]).start()
        fetch(i, row, per).wait()

        def four(q, i=i, per=per):
            base = pl.multiple_of(q * (4 * per), 8)
            for z in range(4):
                flat[pl.ds(base + per * z, per), :] = came[i % 2, *_xy(q), z, :per].astype(jnp.float32)

        _repeat(16, four)
        rows = outs[i].shape[0]
        first = {"wk": 8, "wv": 9}.get(name, 0)
        buf = {"w_gate": wide.at[0], "w_up": wide.at[1], "w_down": high.at[0], "wo": high.at[1, :rows]}.get(name, qkv)
        step = TILE if rows % TILE == 0 else 512

        def gather(j, buf=buf, tiles=tiles, step=step, first=first):
            at = pl.multiple_of(j * step, step)
            for c in range(tiles):
                buf[pl.ds(at, step), _lanes(first + c)] = flat[pl.ds(at * tiles + c, step, stride=tiles), :].astype(jnp.bfloat16)

        _repeat(rows // step, gather)
        give(buf.at[:, _lanes(first, tiles)], outs[i], out_sem.at[i])
    for copy in copies:
        copy.wait()


def spread(flat, new_m, new_v, weights, m):
    low, f32, dma = jnp.bfloat16, jnp.float32, pltpu.SemaphoreType.DMA
    hbm, vmem = pl.BlockSpec(memory_space=pl.ANY), pl.BlockSpec(memory_space=pltpu.VMEM)
    shapes = [jax.ShapeDtypeStruct(weights[n].shape, low) for n in PARTS] + [jax.ShapeDtypeStruct(m[n].shape, f32) for n in PARTS] * 2
    d, units = weights["w_gate"].shape
    return pl.pallas_call(
        _spread,
        in_specs=[hbm, vmem, vmem],
        out_specs=[hbm] * len(shapes),
        out_shape=shapes,
        scratch_shapes=[pltpu.VMEM((2, *CUBE, 256, LANES), low), pltpu.VMEM((64 * 250, LANES), f32), pltpu.VMEM((2, d, units), low),
                        pltpu.VMEM((2, units, d), low), pltpu.VMEM((d, 2 * TILE), low), pltpu.VMEM((2, *m["wo"].shape), f32),
                        dma((2,)), dma((7,)), dma((2, 7))],
        compiler_params=pltpu.CompilerParams(vmem_limit_bytes=64_000_000),
    )(flat, new_m, new_v)


def solution(mesh):
    def step(x, dy, *arrays):
        w, m, v = (dict(zip(NAMES, (one[0] for one in arrays[i : i + 7]))) for i in (0, 7, 14))
        x, dy = x[0], dy[0]
        a, q, k, val, cos, sin, h, b, att, lse = front(x, w["wq"], w["wk"], w["wv"], w["wo"])
        act, by_gate, by_up, by_h, by_att = ffn(b, h, dy, w["w_gate"], w["w_up"], w["w_down"], w["wo"])
        by_qkv = attend_bwd(q, k, val, cos, sin, by_att, att, lse)

        lined = lambda of: {n: one if n == "wo" else one.reshape(-1, 1, LANES) for n, one in of.items()}
        m_lined = lined(m)
        flat = tail({n: w[n] for n in PARTS}, m_lined, lined(v), a=a, b=b, act=act, att=att, dy=dy, by_h=by_h, by_gate=by_gate, by_up=by_up, by_qkv=by_qkv)
        outs = spread(*flat, w, m_lined)
        new = [dict(zip(PARTS, outs[i : i + 7])) for i in (0, 7, 14)]
        return tuple(one[n].reshape(1, *like[n].shape) for one, like in zip(new, (w, m, m)) for n in NAMES)

    states, all_of, cut = P(("rep", "dp")), P(), P(None, "dp")
    return jax.shard_map(
        step,
        mesh=mesh,
        in_specs=(states, states) + (all_of,) * 7 + (cut,) * 14,
        out_specs=(P("rep"),) * 7 + (P("rep", "dp"),) * 14,
        check_vma=False,
    )
```
